32 devices in a mesh: dp: 8 (over z, core), mp: 4 (over y, x).
Axes of the slice: x: 2, y: 2, z: 4, core: 2. Of those that a mesh axis runs over, the one named last changes fastest.
Arguments:
- patches: bfloat16 [256, 256, 1280], P(('dp', 'mp')), may hold values from -6 to 6
- position: bfloat16 [256, 1280], replicated, may hold values from -3 to 3
- keep: int32 [256, 64], P(('dp', 'mp')), may hold values from 0 to 255, as said below
- counts: int32 [256], replicated, may hold values from 1 to 64, as said below
- offsets: int32 [256], replicated, may hold values from 0 to 10239, as said below
- ln_gain: float32 [1, 2, 1280], replicated, may hold values from 0.25 to 1.75
- ln_bias: float32 [1, 2, 1280], replicated, may hold values from -2 to 2
- w_qkv: bfloat16 [1, 3, 1280, 1280], P(None, None, 'dp', 'mp')
- b_qkv: float32 [1, 3, 1280], P(None, None, 'mp'), may hold values from -3 to 3
- w_o: bfloat16 [1, 1280, 1280], P(None, 'mp', 'dp'), may hold values from -0.15625 to 0.15625
- b_o: float32 [1, 1280], replicated, may hold values from -1.5 to 1.5
- w_up: bfloat16 [1, 1280, 5120], P(None, 'dp', 'mp'), may hold values from -0.15625 to 0.15625
- b_up: float32 [1, 5120], P(None, 'mp'), may hold values from -3 to 3
- w_down: bfloat16 [1, 5120, 1280], P(None, 'mp', 'dp'), may hold values from -0.078125 to 0.078125
- b_down: float32 [1, 1280], replicated, may hold values from -1.5 to 1.5
Outputs:
- encoded: bfloat16 [10240, 1280], P(('dp', 'mp'))
The draws below stay inside these ranges and needn't reach their ends.
Inputs may be any that keep to these rules, and one draw needn't show every extreme that they name: `keep`: the first counts[i] entries of row i are distinct and name image i's visible patches; later entries are unused. `counts`: some image has exactly 64 visible patches. Image i, held by dp index s = i // 32, occupies packed rows offsets[i] to offsets[i] + counts[i] - 1, all inside the aligned block of 160 rows numbered d * 8 + s for some shard d; no two images share a row.
All inputs are finite; a program needn't handle non-finite values.
Results may differ from the reference program's by a relative error of at most 0.015.
Values may be sent and summed in bfloat16 or wider, within the bound.
A program may use at most 64 MiB of HBM per device.

```python
import math
import jax
import jax.numpy as jnp
from jax import lax

D = 1280
HEADS = 16
HEAD = 80
FF = 5120
PATCHES = 256
KEEP_MAX = 64
LAYERS = 1
IMG_DEV = 32
IMAGES = 256
SLOT = 160
PACK_DEV = 1280
PACKED = 10240
N_MP = 4


def packing_plan(key):
    shard_total = IMAGES // IMG_DEV
    key_order, key_raw, key_cap, key_force = jax.random.split(jax.random.fold_in(key, 71), 4)
    order = jax.vmap(lambda subkey: jax.random.permutation(subkey, IMG_DEV))(jax.random.split(key_order, shard_total)).astype(jnp.int32)
    destination = order % shard_total
    rank_in = order // shard_total
    lowest = max(1, KEEP_MAX // 8)
    ceiling = jax.random.randint(key_cap, (shard_total, 1), lowest, KEEP_MAX + 1)
    raw_count = jnp.minimum(jax.random.randint(key_raw, (shard_total, IMG_DEV), lowest, KEEP_MAX + 1), ceiling)
    mates = destination[:, :, None] == destination[:, None, :]
    mate_total = jnp.sum(jnp.where(mates, raw_count[:, None, :], 0), axis=-1)
    mate_number = jnp.sum(mates.astype(jnp.int32), axis=-1)
    room = SLOT - mate_number
    scaled = 1 + (raw_count - 1) * room // jnp.maximum(mate_total - mate_number, room)
    forced_source = jax.random.randint(key_force, (), 0, shard_total)
    source_ids = jnp.arange(shard_total, dtype=jnp.int32)[:, None]
    in_source = source_ids == forced_source
    chosen = in_source & (order == 0)
    partner = in_source & (destination == 0)
    counts_grid = jnp.where(chosen, KEEP_MAX, jnp.where(partner, 1, scaled))
    earlier = mates & (rank_in[:, None, :] < rank_in[:, :, None])
    before = jnp.sum(jnp.where(earlier, counts_grid[:, None, :], 0), axis=-1)
    offsets_grid = destination * PACK_DEV + source_ids * SLOT + before
    return (counts_grid.reshape(IMAGES).astype(jnp.int32), offsets_grid.reshape(IMAGES).astype(jnp.int32))


def draw_counts(key, part):
    return packing_plan(key)[0]


def draw_offsets(key, part):
    return packing_plan(key)[1]


def draw_keep(key, part):
    subkeys = jax.random.split(jax.random.fold_in(key, 13), IMAGES)
    return jax.vmap(lambda subkey: jax.random.permutation(subkey, PATCHES)[:KEEP_MAX])(subkeys).astype(jnp.int32)


def draw_w_qkv(key, part):
    key_base = jax.random.fold_in(jax.random.fold_in(key, 29), 0)
    matrices = jax.random.normal(key_base, (LAYERS, 3, D, D), jnp.float32) / math.sqrt(D)
    return matrices.astype(jnp.bfloat16)


def levels(rng, extent, cuts, low, largest):
    level, own = 1.0, jax.random.fold_in(rng, 6)
    for dim, blocks in cuts:
        steps = jnp.exp(jax.random.uniform(jax.random.fold_in(own, dim), (blocks,), jnp.float32, low / len(cuts), largest / len(cuts)))
        level = level * jnp.repeat(steps, extent[dim] // blocks).reshape([-1 if axis == dim else 1 for axis in range(len(extent))])
    return level


def bell_draw(rng, extent, deviation, limit, cuts=(), kind=jnp.bfloat16):
    result = jax.random.normal(rng, extent, jnp.float32) * deviation
    if len(cuts) > 0:
        result = levels(rng, extent, cuts, -0.22, 0.18) * result
    return jnp.clip(result, min=-limit, max=limit).astype(kind)


def setup_inputs(seed: int = 0) -> dict:
    keys = jax.random.split(jax.random.key(seed), 16)
    return {
        "patches": bell_draw(keys[0], (IMAGES, PATCHES, D), 1.0, 6.0, ((0, 32),)),
        "position": bell_draw(keys[1], (PATCHES, D), 0.5, 3.0),
        "keep": draw_keep(jax.random.fold_in(keys[15], 71), 0),
        "counts": draw_counts(jax.random.fold_in(keys[15], 71), 0),
        "offsets": draw_offsets(jax.random.fold_in(keys[15], 71), 0),
        "ln_gain": jnp.clip(1.0 + 0.15 * jax.random.normal(keys[5], (LAYERS, 2, D), jnp.float32), 0.25, 1.75),
        "ln_bias": bell_draw(keys[6], (LAYERS, 2, D), 0.3, 2.0, (), jnp.float32),
        "w_qkv": draw_w_qkv(jax.random.fold_in(keys[15], 71), 0),
        "b_qkv": bell_draw(keys[8], (LAYERS, 3, D), 0.5, 3.0, ((2, 4),), jnp.float32),
        "w_o": bell_draw(keys[9], (LAYERS, D, D), D ** -0.5, 0.15625, ((1, 4), (2, 8))),
        "b_o": bell_draw(keys[10], (LAYERS, D), 0.2, 1.5, (), jnp.float32),
        "w_up": bell_draw(keys[11], (LAYERS, D, FF), D ** -0.5, 0.15625, ((1, 8), (2, 4))),
        "b_up": bell_draw(keys[12], (LAYERS, FF), 0.5, 3.0, ((1, 4),), jnp.float32),
        "w_down": bell_draw(keys[13], (LAYERS, FF, D), FF ** -0.5, 0.078125, ((1, 4), (2, 8))),
        "b_down": bell_draw(keys[14], (LAYERS, D), 0.2, 1.5, (), jnp.float32),
    }


def layer_norm(values, gain_row, shift_row):
    row_mean = lax.optimization_barrier(jnp.mean(values, axis=-1, keepdims=True))
    centred = values - row_mean
    spread = lax.optimization_barrier(jnp.mean(centred * centred, axis=-1, keepdims=True))
    return (centred * lax.rsqrt(spread + 1e-06) * gain_row + shift_row).astype(jnp.bfloat16)

def split_sum(left, weight, groups):
    group_width = left.shape[1] // groups
    running = jnp.zeros((left.shape[0], weight.shape[1]), jnp.float32)
    for group_index in range(groups):
        partial_value = jnp.dot(left[:, group_index * group_width:(group_index + 1) * group_width], weight[group_index * group_width:(group_index + 1) * group_width], preferred_element_type=jnp.float32)
        rounded = lax.optimization_barrier(partial_value.astype(jnp.bfloat16))
        running = running + rounded.astype(jnp.float32)
    return running

def shard_attention(pieces):
    queries, key_rows, value_rows, labels_shard = pieces
    scores = jnp.einsum('qhe,khe->hqk', queries.astype(jnp.float32), key_rows.astype(jnp.float32)) * (1.0 / math.sqrt(HEAD))
    matches = labels_shard[:, None] == labels_shard[None, :]
    scores = jnp.where(matches[None], scores, -jnp.inf)
    row_max = lax.optimization_barrier(jnp.max(scores, axis=-1, keepdims=True))
    weights = jnp.exp(scores - row_max)
    probabilities = (weights / lax.optimization_barrier(jnp.sum(weights, axis=-1, keepdims=True))).astype(jnp.bfloat16)
    attended = jnp.einsum('hqk,khe->qhe', probabilities.astype(jnp.float32), value_rows.astype(jnp.float32))
    return attended.astype(jnp.bfloat16)

def reference(patches, position, keep, counts, offsets, ln_gain, ln_bias, w_qkv, b_qkv, w_o, b_o, w_up, b_up, w_down, b_down):
    picked = jnp.take_along_axis(patches, keep[:, :, None], axis=1)
    placed = jnp.take(position, keep, axis=0)
    tokens = (picked.astype(jnp.float32) + placed.astype(jnp.float32)).astype(jnp.bfloat16)
    positions_in = jnp.arange(KEEP_MAX, dtype=jnp.int32)
    is_live = positions_in[None, :] < counts[:, None]
    target = jnp.where(is_live, offsets[:, None] + positions_in[None, :], PACKED).reshape(-1)
    stream = jnp.zeros((PACKED, D), jnp.bfloat16).at[target].set(tokens.reshape(-1, D), mode='drop')
    packed_rows = jnp.arange(PACKED, dtype=jnp.int32)
    image_ids = jnp.arange(counts.shape[0], dtype=jnp.int32)
    inside = (packed_rows[:, None] >= offsets[None, :]) & (packed_rows[:, None] < (offsets + counts)[None, :])
    labels = lax.optimization_barrier(jnp.max(jnp.where(inside, image_ids[None, :] + 1, 0), axis=1)) - 1
    shard_total = PACKED // PACK_DEV
    for layer_index in range(LAYERS):
        normed = layer_norm(stream.astype(jnp.float32), ln_gain[layer_index, 0], ln_bias[layer_index, 0])
        projected = (jnp.einsum('rd,tdc->trc', normed.astype(jnp.float32), w_qkv[layer_index].astype(jnp.float32)) + b_qkv[layer_index][:, None, :]).astype(jnp.bfloat16)
        shaped = projected.reshape(3, shard_total, PACK_DEV, HEADS, HEAD)
        attended = lax.map(shard_attention, (shaped[0], shaped[1], shaped[2], labels.reshape(shard_total, PACK_DEV)))
        attended = attended.reshape(PACKED, D)
        residual = stream.astype(jnp.float32) + split_sum(attended, w_o[layer_index], N_MP) + b_o[layer_index]
        normed_mlp = layer_norm(residual, ln_gain[layer_index, 1], ln_bias[layer_index, 1])
        up_proj = jnp.dot(normed_mlp, w_up[layer_index], preferred_element_type=jnp.float32) + b_up[layer_index]
        hidden = jax.nn.gelu(up_proj, approximate=False).astype(jnp.bfloat16)
        stream = (residual + split_sum(hidden, w_down[layer_index], N_MP) + b_down[layer_index]).astype(jnp.bfloat16)
    return jnp.where(labels[:, None] >= 0, stream, jnp.zeros_like(stream))
```

```python
import functools
import math

import jax
import jax.numpy as jnp
from jax import lax
from jax.experimental import pallas as pl
from jax.experimental.pallas import tpu as pltpu
from jax.sharding import PartitionSpec as P

HEAD = 80
MESH = pl.DeviceIdType.MESH


def norm_rows(values, gain_row, shift_row):
    row_mean = jnp.mean(values, axis=-1, keepdims=True)
    centred = values - row_mean
    spread = jnp.mean(centred * centred, axis=-1, keepdims=True)
    return (centred * lax.rsqrt(spread + 1e-06) * gain_row + shift_row).astype(jnp.bfloat16)


def flip(index, mask, count):
    result = index
    bit = 1
    while bit < count:
        wanted = (mask // bit) % 2
        own = (index // bit) % 2
        result = result + bit * wanted * (1 - 2 * own)
        bit = bit * 2
    return result


def tile_of(extent, most):
    tile = most
    while extent % tile != 0:
        tile = tile // 2
    return tile


def route_kernel(
    shards,
    groups,
    packed_ref,
    gain_ref,
    shift_ref,
    stream_ref,
    normed_ref,
    out_ref,
    send_sem,
    recv_sem,
    own_sem,
):
    per = shards // groups
    dp = lax.axis_index("dp")
    mp = lax.axis_index("mp")
    home = dp // per
    slot = lax.rem(dp, per) * groups + mp

    barrier = pltpu.get_barrier_semaphore()
    for j in range(per):
        for g in range(groups):
            source = mp * per + j

            @pl.when(jnp.logical_or(source != dp, mp != g))
            def _():
                pl.semaphore_signal(barrier, inc=1, device_id=(source, g), device_id_type=MESH)

    is_home = home == mp

    @pl.when(is_home)
    def _():
        pl.semaphore_wait(barrier, shards - 1)

    @pl.when(jnp.logical_not(is_home))
    def _():
        pl.semaphore_wait(barrier, shards)

    def remote(step):
        dest = lax.rem(dp + step, shards)
        return pltpu.make_async_remote_copy(
            src_ref=packed_ref.at[dest],
            dst_ref=out_ref.at[slot],
            send_sem=send_sem.at[step],
            recv_sem=recv_sem.at[slot],
            device_id=(dest, home),
            device_id_type=MESH,
        )

    own = pltpu.make_async_copy(packed_ref.at[dp], out_ref.at[slot], own_sem)
    for step in range(1, shards):
        remote(step).start()

    @pl.when(is_home)
    def _():
        own.start()
        own.wait()

    @pl.when(jnp.logical_not(is_home))
    def _():
        remote(0).start()
        remote(0).wait_send()

    for step in range(1, shards):
        remote(step).wait_send()
    for j in range(per):
        for g in range(groups):
            source = mp * per + j

            @pl.when(jnp.logical_or(source != dp, mp != g))
            def _():
                pltpu.make_async_remote_copy(
                    src_ref=packed_ref.at[0],
                    dst_ref=out_ref.at[j * groups + g],
                    send_sem=send_sem.at[0],
                    recv_sem=recv_sem.at[j * groups + g],
                    device_id=(dp, mp),
                    device_id_type=MESH,
                ).wait_recv()

    rows_tile = tile_of(packed_ref.shape[1], 32)
    for j in range(per):

        def some(i, carry):
            rows = pl.ds(pl.multiple_of(i * rows_tile, rows_tile), rows_tile)
            whole = jnp.concatenate(
                [out_ref[j * groups + g, rows, :] for g in range(groups)], axis=-1
            )
            stream_ref[j, rows, :] = whole
            normed_ref[j, rows, :] = norm_rows(
                whole.astype(jnp.float32), gain_ref[...], shift_ref[...]
            )
            return carry

        lax.fori_loop(0, packed_ref.shape[1] // rows_tile, some, 0)


def route(packed, gain_row, shift_row, shards, groups):
    slot_rows, width = packed.shape[1:]
    result = jax.ShapeDtypeStruct((shards // groups, slot_rows, width * groups), packed.dtype)
    vmem = pl.BlockSpec(memory_space=pltpu.VMEM)
    return pl.pallas_call(
        functools.partial(route_kernel, shards, groups),
        out_shape=(result, result),
        in_specs=[vmem] * 3,
        out_specs=(vmem, vmem),
        scratch_shapes=[
            pltpu.VMEM(packed.shape, packed.dtype),
            pltpu.SemaphoreType.DMA((shards,)),
            pltpu.SemaphoreType.DMA((shards,)),
            pltpu.SemaphoreType.DMA,
        ],
        compiler_params=pltpu.CompilerParams(collective_id=0, has_side_effects=True),
        cost_estimate=pl.CostEstimate(flops=15_000_000_000, bytes_accessed=0, transcendentals=0),
        name="route",
    )(packed, gain_row, shift_row)


def exchange(groups, x_ref, blocks, parts, backs, relay, sems, block_step, finish):
    own_sem, send_a, recv_a, send_b, recv_b = sems
    dp = lax.axis_index("dp")
    mp = lax.axis_index("mp")
    pieces = x_ref.shape[0]
    square = groups == 4 and pieces == 2
    partners = range(1, 3) if square else range(1, groups)

    barrier = pltpu.get_barrier_semaphore()
    for k in partners:
        pl.semaphore_signal(
            barrier, inc=1, device_id=(dp, flip(mp, k, groups)), device_id_type=MESH
        )
    own = pltpu.make_async_copy(x_ref, blocks.at[pl.ds(0, pieces)], own_sem)
    own.start()
    pl.semaphore_wait(barrier, len(partners))

    def send(source, target, out_sem, in_sem, k):
        return pltpu.make_async_remote_copy(
            src_ref=source,
            dst_ref=target,
            send_sem=out_sem,
            recv_sem=in_sem,
            device_id=(dp, flip(mp, k, groups)),
            device_id_type=MESH,
        )

    def out_copy(k, h):
        at = k * pieces + h
        return send(x_ref.at[h], blocks.at[at], send_a.at[at], recv_a.at[at], k)

    def back_copy(k, h):
        at = k * pieces + h
        return send(parts.at[at], backs.at[at], send_b.at[at], recv_b.at[at], k)

    if square:
        def forward(h):
            held, k = (2, 2) if h == 0 else (5, 1)
            at = 6 + h
            return send(blocks.at[held], blocks.at[at], send_a.at[at], recv_a.at[at], k)

        def across(h):
            at = 6 + h
            return send(parts.at[at], relay.at[h], send_b.at[at], recv_b.at[at], 1 + h)

        for k, h in ((1, 0), (2, 1), (1, 1), (2, 0)):
            out_copy(k, h).start()
        own.wait()

        def step(i, carry):
            late = (i + 2) // 8
            middle = ((i + 2) // 4) % 2
            k = middle * (1 + i % 2) + 3 * late
            h = (i // 4 + i % 2) % 2

            @pl.when(i == 2)
            def _():
                out_copy(1, 0).wait_recv()
                forward(0).start()
                out_copy(2, 1).wait_recv()
                forward(1).start()

            @pl.when(i >= 4)
            def _():
                out_copy(k, h).wait_recv()

            block_step(k * 2 + h, flip(mp, k, groups) * 2 + h)

            @pl.when(i == 2)
            def _():
                back_copy(1, 0).start()

            @pl.when(i == 3)
            def _():
                back_copy(2, 1).start()

            @pl.when(i == 6)
            def _():
                across(1).start()

            @pl.when(i == 7)
            def _():
                across(0).start()

            return carry

        lax.fori_loop(0, 8, step, 0)
        rows_tile = tile_of(x_ref.shape[1], 32)
        for h, k in ((1, 1), (0, 2)):
            across(h).wait_recv()

            def add(i, carry, h=h, k=k):
                rows = pl.ds(pl.multiple_of(i * rows_tile, rows_tile), rows_tile)
                parts[k * 2 + h, rows, :] = (
                    parts[k * 2 + h, rows, :].astype(jnp.float32)
                    + relay[h, rows, :].astype(jnp.float32)
                ).astype(jnp.bfloat16)
                return carry

            lax.fori_loop(0, x_ref.shape[1] // rows_tile, add, 0)
            back_copy(k, h).start()
        for k, h in ((1, 0), (2, 1), (1, 1), (2, 0)):
            back_copy(k, h).wait_recv()
        finish(partners)
        for h in range(2):
            forward(h).wait_send()
            across(h).wait_send()
            for k in partners:
                out_copy(k, h).wait_send()
                back_copy(k, h).wait_send()
        return

    for k in partners:
        for h in range(pieces):
            out_copy(k, h).start()
    own.wait()

    def step(i, carry):
        k = i // pieces
        h = i % pieces

        @pl.when(k > 0)
        def _():
            out_copy(k, h).wait_recv()

        block_step(i, flip(mp, k, groups) * pieces + h)

        @pl.when(k > 0)
        def _():
            back_copy(k, h).start()

        return carry

    lax.fori_loop(0, groups * pieces, step, 0)
    for k in partners:
        for h in range(pieces):
            back_copy(k, h).wait_recv()
    finish(partners)
    for k in partners:
        for h in range(pieces):
            out_copy(k, h).wait_send()
            back_copy(k, h).wait_send()


def finish_rows(x_ref, parts, backs, partners, write):
    pieces, row_count = x_ref.shape[:2]
    rows_tile = tile_of(row_count, 32)
    for h in range(pieces):

        def some(i, carry, h=h):
            rows = pl.ds(pl.multiple_of(i * rows_tile, rows_tile), rows_tile)
            total = parts[h, rows, :].astype(jnp.float32)
            for k in partners:
                total = total + backs[k * pieces + h, rows, :].astype(jnp.float32)
            write(h, rows, total)
            return carry

        lax.fori_loop(0, row_count // rows_tile, some, 0)


def attention_kernel(
    groups,
    x_ref,
    stream_ref,
    w_ref,
    b_ref,
    label_col_ref,
    label_row_ref,
    bias_ref,
    gain_ref,
    shift_ref,
    residual_ref,
    normed_ref,
    blocks,
    parts,
    backs,
    relay,
    attended_ref,
    *sems,
):
    row_count, depth = x_ref.shape[1:]
    width = w_ref.shape[2]
    heads = width // HEAD
    scale = 1.0 / math.sqrt(HEAD)
    tile = tile_of(depth, 256)

    def block_step(at_block, source):
        x = blocks[at_block]

        def project(t):
            y = jnp.dot(x, w_ref[t], preferred_element_type=jnp.float32)
            return (y + b_ref[t]).astype(jnp.bfloat16)

        query, key, value = project(0), project(1), project(2)
        matches = label_col_ref[source] == label_row_ref[source]
        lane_head = lax.broadcasted_iota(jnp.int32, (row_count, width), 1)
        total = jnp.zeros((row_count, width), jnp.float32)
        zero = jnp.zeros((row_count, width), jnp.bfloat16)
        for h in range(heads):
            inside = (lane_head >= h * HEAD) & (lane_head < (h + 1) * HEAD)
            scores = lax.dot_general(
                jnp.where(inside, query, zero),
                key,
                (((1,), (1,)), ((), ())),
                preferred_element_type=jnp.float32,
            )
            scores = jnp.where(matches, scores * scale, -jnp.inf)
            weights = jnp.exp(scores - jnp.max(scores, axis=-1, keepdims=True))
            inverse = 1.0 / jnp.sum(weights, axis=-1, keepdims=True)
            probabilities = (weights * inverse).astype(jnp.bfloat16)
            total = total + jnp.dot(
                probabilities, jnp.where(inside, value, zero), preferred_element_type=jnp.float32
            )
        attended_ref[...] = total.astype(jnp.bfloat16)

        def column(t, carry):
            at = pl.ds(pl.multiple_of(t * tile, tile), tile)
            parts[at_block, :, at] = lax.dot_general(
                attended_ref[...],
                w_ref[3, at, :],
                (((1,), (1,)), ((), ())),
                preferred_element_type=jnp.float32,
            ).astype(jnp.bfloat16)
            return carry

        lax.fori_loop(0, depth // tile, column, 0)

    def finish(partners):
        def write(h, rows, total):
            residual = stream_ref[h, rows, :].astype(jnp.float32) + total + bias_ref[...]
            residual_ref[h, rows, :] = residual
            normed_ref[h, rows, :] = norm_rows(residual, gain_ref[...], shift_ref[...])

        finish_rows(x_ref, parts, backs, partners, write)

    exchange(groups, x_ref, blocks, parts, backs, relay, sems, block_step, finish)


def mlp_kernel(
    groups,
    x_ref,
    residual_ref,
    up_ref,
    b_ref,
    down_ref,
    bias_ref,
    out_ref,
    blocks,
    parts,
    backs,
    relay,
    hidden_ref,
    *sems,
):
    row_count, depth = x_ref.shape[1:]
    width = up_ref.shape[1]
    tile = tile_of(depth, 256)
    up_tile = tile_of(width, 256)

    def block_step(at_block, source):
        def up(t, carry):
            at = pl.ds(pl.multiple_of(t * up_tile, up_tile), up_tile)
            y = jnp.dot(blocks[at_block], up_ref[:, at], preferred_element_type=jnp.float32) + b_ref[:, at]
            y = 0.5 * y * (1.0 + lax.erf(y * math.sqrt(0.5)))
            hidden_ref[:, at] = y.astype(jnp.bfloat16)
            return carry

        lax.fori_loop(0, width // up_tile, up, 0)

        def column(t, carry):
            at = pl.ds(pl.multiple_of(t * tile, tile), tile)
            parts[at_block, :, at] = lax.dot_general(
                hidden_ref[...],
                down_ref[at, :],
                (((1,), (1,)), ((), ())),
                preferred_element_type=jnp.float32,
            ).astype(jnp.bfloat16)
            return carry

        lax.fori_loop(0, depth // tile, column, 0)

    def finish(partners):
        def write(h, rows, total):
            out_ref[h, rows, :] = (residual_ref[h, rows, :] + total + bias_ref[...]).astype(
                jnp.bfloat16
            )

        finish_rows(x_ref, parts, backs, partners, write)

    exchange(groups, x_ref, blocks, parts, backs, relay, sems, block_step, finish)


def exchange_call(kernel, groups, args, outs, width, collective_id, name):
    pieces, row_count, depth = args[0].shape
    vmem = pl.BlockSpec(memory_space=pltpu.VMEM)
    many = pltpu.SemaphoreType.DMA((groups * pieces,))
    buffer = pltpu.VMEM((groups * pieces, row_count, depth), jnp.bfloat16)
    return pl.pallas_call(
        functools.partial(kernel, groups),
        out_shape=outs,
        in_specs=[vmem] * len(args),
        out_specs=jax.tree.map(lambda _: vmem, outs),
        scratch_shapes=[
            buffer,
            buffer,
            buffer,
            pltpu.VMEM((pieces, row_count, depth), jnp.bfloat16),
            pltpu.VMEM((row_count, width), jnp.bfloat16),
            pltpu.SemaphoreType.DMA,
            many,
            many,
            many,
            many,
        ],
        compiler_params=pltpu.CompilerParams(
            collective_id=collective_id, has_side_effects=True, vmem_limit_bytes=48 * 1024 * 1024
        ),
        cost_estimate=pl.CostEstimate(flops=50_000_000_000, bytes_accessed=0, transcendentals=0),
        name=name,
    )(*args)

def slot_size(images_here, shards, keep_most):
    per_slot = (images_here + shards - 1) // shards
    return max(keep_most + 16, per_slot * keep_most * 5 // 8)


def per_device(
    patches,
    position,
    keep,
    counts,
    offsets,
    ln_gain,
    ln_bias,
    w_qkv,
    b_qkv,
    w_o,
    b_o,
    w_up,
    b_up,
    w_down,
    b_down,
):
    local_images, patch_count, column_count = patches.shape
    keep_most = keep.shape[1]
    shard_count = lax.axis_size("dp")
    group_size = lax.axis_size("mp")
    images_here = local_images * group_size
    slot_rows = slot_size(images_here, shard_count, keep_most)
    pack_rows = slot_rows * shard_count
    local_rows = pack_rows // group_size
    dp_index = lax.axis_index("dp")
    mp_index = lax.axis_index("mp")
    f32 = jnp.float32

    attention_shard = jnp.concatenate([w_qkv[0], w_o[0].T[None]], axis=0)
    w_attention = lax.all_gather(attention_shard, "dp", axis=1, tiled=True)

    chosen = (keep[:, :, None] == jnp.arange(patch_count, dtype=jnp.int32)).astype(jnp.bfloat16)
    tokens = (
        jnp.einsum("ijp,ipd->ijd", chosen, patches, preferred_element_type=f32)
        + jnp.einsum("ijp,pd->ijd", chosen, position, preferred_element_type=f32)
    ).astype(jnp.bfloat16)
    tokens, w_up_shard = lax.optimization_barrier((tokens, w_up[0]))
    w_up_full = lax.all_gather(w_up_shard, "dp", axis=0, tiled=True)

    first_image = dp_index * images_here
    group_counts = lax.dynamic_slice_in_dim(counts, first_image, images_here)
    group_offsets = lax.dynamic_slice_in_dim(offsets, first_image, images_here)
    positions_in = jnp.arange(keep_most, dtype=jnp.int32)
    group_live = positions_in[None, :] < group_counts[:, None]
    shard_index = group_offsets // pack_rows
    base_row = (
        shard_index * slot_rows + group_offsets - shard_index * pack_rows - dp_index * slot_rows
    )
    target = jnp.where(group_live, base_row[:, None] + positions_in[None, :], pack_rows).reshape(-1)
    image_ids = jnp.arange(counts.shape[0], dtype=jnp.int32)
    packed_rows = dp_index * pack_rows + jnp.arange(pack_rows, dtype=jnp.int32)
    inside = (packed_rows[:, None] >= offsets[None, :]) & (
        packed_rows[:, None] < (offsets + counts)[None, :]
    )
    labels = jnp.max(jnp.where(inside, image_ids[None, :] + 1, 0), axis=1) - 1

    featured = lax.all_to_all(
        tokens.reshape(-1, column_count), "mp", split_axis=1, concat_axis=0, tiled=True
    )
    featured, w_down_shard = lax.optimization_barrier((featured, w_down[0]))
    w_down_rows = lax.all_gather(w_down_shard, "dp", axis=1, tiled=True).T
    feature_count = featured.shape[1]
    placing = (jnp.arange(pack_rows, dtype=jnp.int32)[:, None] == target[None, :]).astype(
        jnp.bfloat16
    )
    packed = jnp.dot(placing, featured, preferred_element_type=f32).astype(jnp.bfloat16)
    stream, normed = route(
        packed.reshape(shard_count, slot_rows, feature_count),
        ln_gain[:, 0],
        ln_bias[:, 0],
        shard_count,
        group_size,
    )
    pieces = stream.shape[0]
    by_piece = labels.reshape(group_size * pieces, local_rows // pieces)
    residual, normed_mlp = exchange_call(
        attention_kernel,
        group_size,
        (
            normed,
            stream,
            w_attention,
            b_qkv[0][:, None, :],
            by_piece[:, :, None],
            by_piece[:, None, :],
            b_o,
            ln_gain[:, 1],
            ln_bias[:, 1],
        ),
        (
            jax.ShapeDtypeStruct(stream.shape, f32),
            jax.ShapeDtypeStruct(stream.shape, jnp.bfloat16),
        ),
        w_attention.shape[2],
        1,
        "attention",
    )
    stream = exchange_call(
        mlp_kernel,
        group_size,
        (normed_mlp, residual, w_up_full, b_up, w_down_rows, b_down),
        jax.ShapeDtypeStruct(stream.shape, jnp.bfloat16),
        w_up_full.shape[1],
        2,
        "mlp",
    ).reshape(local_rows, column_count)
    own_labels = lax.dynamic_slice_in_dim(labels, mp_index * local_rows, local_rows)
    return jnp.where(own_labels[:, None] >= 0, stream, jnp.zeros_like(stream))

def by_pair(index, values):
    low = index % 2
    high = index // 2
    return (
        values[0] * (1 - low) * (1 - high)
        + values[1] * low * (1 - high)
        + values[2] * (1 - low) * high
        + values[3] * low * high
    )


ARRIVALS = ((0, 1, 2, 3), (1, 0, 2, 3), (2, 1, 3, 0), (3, 2, 1, 0))


def layer_kernel(
    shards,
    groups,
    patches_ref,
    position_ref,
    keep_ref,
    target_ref,
    label_col_ref,
    label_row_ref,
    gain_ref,
    shift_ref,
    attention_shard_ref,
    b_attention_ref,
    b_o_ref,
    mlp_shard_ref,
    b_up_ref,
    b_down_ref,
    out_ref,
    patch_buf,
    token_out,
    token_in,
    slot_out,
    slot_in,
    w_attention,
    b_attention,
    w_mlp,
    normed_ref,
    projected_ref,
    attended_ref,
    residual_ref,
    blocks,
    parts,
    backs,
    relay,
    hidden_ref,
    patch_sem,
    local_sem,
    token_send,
    token_recv,
    slot_send,
    slot_recv,
    bias_send,
    bias_recv,
    att_up,
    att_down,
    att_plane,
    att_twin,
    att_recv,
    att_twin_recv,
    mlp_up,
    mlp_down,
    mlp_twin,
    mlp_recv,
    mlp_twin_recv,
    send_a,
    recv_a,
    send_b,
    recv_b,
):
    f32 = jnp.float32
    bf16 = jnp.bfloat16
    dp = lax.axis_index("dp")
    mp = lax.axis_index("mp")
    per = shards // groups
    planes = shards // 2
    z = dp // 2
    core = dp % 2
    home = dp // per
    images, patch_count, depth = patches_ref.shape
    keep_most = keep_ref.shape[1]
    feature = depth // groups
    pieces, piece_rows = blocks.shape[1:3]
    shard_rows = attention_shard_ref.shape[0]
    half_images = images // 2
    last = planes - 1

    def remote(source, target, out_sem, in_sem, device):
        return pltpu.make_async_remote_copy(
            src_ref=source,
            dst_ref=target,
            send_sem=out_sem,
            recv_sem=in_sem,
            device_id=device,
            device_id_type=MESH,
        )

    def peer(k):
        return (dp, flip(mp, k, groups))

    twin = (dp + 1 - 2 * core, mp)
    above = (lax.rem(dp + 2, shards), mp)
    below = (lax.rem(dp + shards - 2, shards), mp)

    for i in range(images):
        pltpu.make_async_copy(patches_ref.at[i], patch_buf.at[i], patch_sem.at[i]).start()

    barrier = pltpu.get_barrier_semaphore()
    for j in range(per):
        for g in range(groups):
            source = mp * per + j

            @pl.when(jnp.logical_or(source != dp, mp != g))
            def _():
                pl.semaphore_signal(barrier, inc=1, device_id=(source, g), device_id_type=MESH)

    for k in range(1, groups):
        pl.semaphore_signal(barrier, inc=1, device_id=peer(k), device_id_type=MESH)
    pl.semaphore_signal(barrier, inc=1, device_id=twin, device_id_type=MESH)

    @pl.when(z < last)
    def _():
        pl.semaphore_signal(barrier, inc=1, device_id=above, device_id_type=MESH)

    @pl.when(z > 0)
    def _():
        pl.semaphore_signal(barrier, inc=1, device_id=below, device_id_type=MESH)

    own_rows = pl.ds(pl.multiple_of(dp * shard_rows, 16), shard_rows)
    own_att = pltpu.make_async_copy(
        attention_shard_ref, w_attention.at[mp, own_rows, :], local_sem.at[0]
    )
    own_mlp = pltpu.make_async_copy(mlp_shard_ref, w_mlp.at[:, own_rows, :], local_sem.at[1])
    own_bias = pltpu.make_async_copy(b_attention_ref, b_attention.at[mp], local_sem.at[2])
    own_att.start()
    own_mlp.start()
    own_bias.start()
    is_home = home == mp
    away = jnp.where(is_home, 0, 1)
    between = jnp.where(jnp.logical_and(z > 0, z < last), 1, 0)
    pl.semaphore_wait(barrier, shards + groups + away + between)

    own_att.wait()
    own_mlp.wait()
    own_bias.wait()

    def rows_of(plane):
        return pl.ds(pl.multiple_of((2 * plane + core) * shard_rows, 16), shard_rows)

    def att_copy(group, plane, out_sem, device):
        at = w_attention.at[group, rows_of(plane), :]
        return remote(at, at, out_sem, att_recv.at[group * planes + plane], device)

    def att_to_twin(group, plane):
        at = w_attention.at[group, rows_of(plane), :]
        index = group * planes + plane
        return remote(at, at, att_twin.at[index], att_twin_recv.at[index], twin)

    def att_over(k, group, plane, relayed):
        return att_copy(group, plane, att_plane.at[(k * 2 + relayed) * planes + plane], peer(k))

    def arrival(p):
        return by_pair(z, [row[p] for row in ARRIVALS])

    def att_held(p):
        plane = arrival(p)
        if p > 0:
            att_copy(mp, plane, att_up.at[plane], twin).wait_recv()

        @pl.when(jnp.logical_and(plane <= z, z < last))
        def _():
            att_copy(mp, plane, att_up.at[plane], above).start()

        @pl.when(jnp.logical_and(plane >= z, z > 0))
        def _():
            att_copy(mp, plane, att_down.at[plane], below).start()

        att_to_twin(mp, plane).start()

    def att_spread(p):
        plane = arrival(p)
        for k in (1, 2):
            att_over(k, mp, plane, 0).start()

    def att_near(p):
        plane = arrival(p)
        for k in (1, 2):
            group = flip(mp, k, groups)
            att_copy(group, plane, att_up.at[plane], twin).wait_recv()
            if p % 2 == k - 1:
                att_over(3 - k, group, plane, 1).start()
            att_to_twin(group, plane).start()

    def att_far(p):
        plane = arrival(p)
        group = flip(mp, 3, groups)
        att_copy(group, plane, att_up.at[plane], twin).wait_recv()
        att_to_twin(group, plane).start()

    def mlp_copy(j, plane, out_sem, device):
        at = w_mlp.at[j, rows_of(plane), :]
        return remote(at, at, out_sem, mlp_recv.at[j * planes + plane], device)

    def mlp_to_twin(j, plane):
        at = w_mlp.at[j, rows_of(plane), :]
        index = j * planes + plane
        return remote(at, at, mlp_twin.at[index], mlp_twin_recv.at[index], twin)

    def mlp_held(j, p):
        plane = arrival(p)
        index = j * planes + plane
        if p > 0:
            mlp_copy(j, plane, mlp_up.at[index], twin).wait_recv()

        @pl.when(jnp.logical_and(plane <= z, z < last))
        def _():
            mlp_copy(j, plane, mlp_up.at[index], above).start()

        @pl.when(jnp.logical_and(plane >= z, z > 0))
        def _():
            mlp_copy(j, plane, mlp_down.at[index], below).start()

        mlp_to_twin(j, plane).start()

    def bias_copy(k):
        return remote(
            b_attention.at[mp], b_attention.at[mp], bias_send.at[k], bias_recv.at[mp], peer(k)
        )

    for k in range(1, groups):
        bias_copy(k).start()
    att_held(0)

    def token_copy(g, i):
        rows = pl.ds(pl.multiple_of(i * keep_most, keep_most), keep_most)
        return remote(
            token_out.at[g, rows, :],
            token_in.at[mp, rows, :],
            token_send.at[g * half_images + i],
            token_recv.at[mp * half_images + i],
            (dp, g),
        )

    def own_tokens(i):
        rows = pl.ds(pl.multiple_of(i * keep_most, keep_most), keep_most)
        return pltpu.make_async_copy(
            token_out.at[mp, rows, :],
            token_in.at[mp, rows, :],
            token_recv.at[mp * half_images + i],
        )

    patch_ids = lax.broadcasted_iota(jnp.int32, (keep_most, patch_count), 1)

    def pick(i):
        pltpu.make_async_copy(patches_ref.at[i], patch_buf.at[i], patch_sem.at[i]).wait()
        chosen = (keep_ref[i] == patch_ids).astype(bf16)
        return jnp.dot(chosen, patch_buf[i], preferred_element_type=f32) + jnp.dot(
            chosen, position_ref[...], preferred_element_type=f32
        )

    def some_tokens(i, carry):
        rows = pl.ds(pl.multiple_of(i * keep_most, keep_most), keep_most)
        left = pick(i)
        right = pick(i + half_images)
        for g in range(groups):
            at = slice(g * feature, (g + 1) * feature)
            token_out[g, rows, :] = jnp.concatenate([left[:, at], right[:, at]], axis=-1).astype(
                bf16
            )
        for g in range(groups):

            @pl.when(mp != g)
            def _():
                token_copy(g, i).start()

        own_tokens(i).start()
        return carry

    lax.fori_loop(0, half_images, some_tokens, 0)
    att_spread(0)
    att_held(1)
    att_spread(1)

    def tokens_here(k, carry):
        group = flip(mp, k, groups)

        def one(i, carry):
            remote(
                token_out.at[0, pl.ds(0, keep_most), :],
                token_in.at[group, pl.ds(pl.multiple_of(i * keep_most, keep_most), keep_most), :],
                token_send.at[0],
                token_recv.at[group * half_images + i],
                twin,
            ).wait_recv()
            return carry

        return lax.fori_loop(0, half_images, one, carry)

    for i in range(half_images):
        own_tokens(i).wait()
    lax.fori_loop(1, groups, tokens_here, 0)

    def slot_copy(dest):
        slot = lax.rem(dp, per) * groups + mp
        return remote(
            slot_out.at[dest],
            slot_in.at[slot],
            slot_send.at[dest],
            slot_recv.at[slot],
            (dest, home),
        )

    def own_slot():
        slot = lax.rem(dp, per) * groups + mp
        return pltpu.make_async_copy(slot_out.at[dp], slot_in.at[slot], slot_recv.at[slot])

    slot_rows = 2 * slot_out.shape[1]
    half_rows = slot_out.shape[1]
    token_count = groups * half_images * keep_most
    edge = feature // 128 * 128
    width = feature - edge + feature

    def place(i, carry):
        first = 2 * i * slot_rows
        rows = first + lax.broadcasted_iota(jnp.int32, (2 * slot_rows, token_count), 0)
        left = (rows == target_ref[0]).astype(bf16)
        right = (rows == target_ref[1]).astype(bf16)
        tokens = token_in[...].reshape(token_count, 2 * feature)
        whole = (
            jnp.dot(left, tokens[:, :width], preferred_element_type=f32)[:, :feature]
            + jnp.dot(right, tokens[:, edge:], preferred_element_type=f32)[:, feature - edge :]
        )
        for j in range(2):
            upper = whole[2 * j * half_rows : (2 * j + 1) * half_rows]
            lower = whole[(2 * j + 1) * half_rows : (2 * j + 2) * half_rows]
            slot_out[2 * i + j] = jnp.concatenate([upper, lower], axis=-1).astype(bf16)
        for j in range(2):
            dest = 2 * i + j
            stays = jnp.logical_and(is_home, dest == dp)

            @pl.when(stays)
            def _():
                own_slot().start()

            @pl.when(jnp.logical_not(stays))
            def _():
                slot_copy(dest).start()

        return carry

    lax.fori_loop(0, shards // 2, place, 0)
    att_held(2)
    att_spread(2)
    att_near(0)
    att_held(3)
    att_spread(3)
    mlp_held(0, 0)

    for j in range(per):
        for g in range(groups):
            source = mp * per + j
            stays = jnp.logical_and(source == dp, mp == g)

            @pl.when(stays)
            def _():
                own_slot().wait()

            @pl.when(jnp.logical_not(stays))
            def _():
                remote(
                    slot_out.at[0],
                    slot_in.at[j * groups + g],
                    slot_send.at[0],
                    slot_recv.at[j * groups + g],
                    twin,
                ).wait_recv()

    rows_tile = tile_of(half_rows, 16)
    steps = half_rows // rows_tile

    def assemble(i, carry):
        j = i // (2 * steps)
        half = (i // steps) % 2
        rows = pl.ds(pl.multiple_of((i % steps) * rows_tile, rows_tile), rows_tile)

        def put(low):
            whole = jnp.concatenate(
                [
                    slot_in[j * groups + g, rows, :].astype(f32)[:, low : low + feature]
                    for g in range(groups)
                ],
                axis=-1,
            )
            to = pl.ds(pl.multiple_of(i * rows_tile, rows_tile), rows_tile)
            residual_ref[to, :] = whole + b_o_ref[...]
            normed_ref[to, :] = norm_rows(whole, gain_ref[0:1], shift_ref[0:1])

        @pl.when(half == 0)
        def _():
            put(0)

        @pl.when(half == 1)
        def _():
            put(feature)

        return carry

    lax.fori_loop(0, 2 * per * steps, assemble, 0)
    mlp_held(0, 1)

    heads = feature // HEAD
    scale = 1.0 / math.sqrt(HEAD)
    used = 3 * feature
    total_width = w_attention.shape[2]
    column = 256
    low_out = used // 128 * 128
    low_key = feature // 128 * 128

    def one_group(step, carry):
        group = flip(mp, step, groups)

        @pl.when(step == 1)
        def _():
            mlp_held(0, 2)
            for p in range(1, planes):
                att_near(p)
            mlp_held(0, 3)
            mlp_held(1, 0)
            att_far(0)
            att_far(1)

        @pl.when(step == 2)
        def _():
            mlp_held(1, 1)

        @pl.when(step == 3)
        def _():
            att_far(2)
            att_far(3)
            mlp_held(1, 2)

        @pl.when(step > 0)
        def _():
            remote(
                b_attention.at[0], b_attention.at[group], bias_send.at[0], bias_recv.at[group], twin
            ).wait_recv()

        for plane in range(planes):
            at = w_attention.at[group, pl.ds(0, shard_rows), :]
            remote(
                at, at, att_twin.at[0], att_twin_recv.at[group * planes + plane], twin
            ).wait_recv()

        def project(t, carry):
            at = pl.ds(pl.multiple_of(t * column, column), column)
            y = jnp.dot(normed_ref[...], w_attention[group, :, at], preferred_element_type=f32)
            projected_ref[:, at] = (y + b_attention[group, 0:1, at]).astype(bf16)
            return carry

        lax.fori_loop(0, projected_ref.shape[1] // column, project, 0)

        def one_slot(j, carry):
            rows = pl.ds(pl.multiple_of(j * slot_rows, 16), slot_rows)
            query = projected_ref[rows, 0:feature]
            key = projected_ref[rows, low_key : 2 * feature].astype(f32)[:, feature - low_key :]
            key = key.astype(bf16)
            value = projected_ref[rows, 2 * feature : used]
            matches = label_col_ref[j] == label_row_ref[j]
            spans = [(t, min(t + 128, feature)) for t in range(0, feature, 128)]
            totals = [jnp.zeros((slot_rows, high - low), f32) for low, high in spans]
            for h in range(heads):
                low = h * HEAD // 128 * 128
                high = min(((h + 1) * HEAD + 127) // 128 * 128, feature)
                lane = low + lax.broadcasted_iota(jnp.int32, (slot_rows, high - low), 1)
                inside = (lane >= h * HEAD) & (lane < (h + 1) * HEAD)
                zero = jnp.zeros((slot_rows, high - low), bf16)
                scores = lax.dot_general(
                    jnp.where(inside, query[:, low:high], zero),
                    key[:, low:high],
                    (((1,), (1,)), ((), ())),
                    preferred_element_type=f32,
                )
                scores = jnp.where(matches, scores * scale, -jnp.inf)
                weights = jnp.exp(scores - jnp.max(scores, axis=-1, keepdims=True))
                inverse = 1.0 / jnp.sum(weights, axis=-1, keepdims=True)
                probabilities = (weights * inverse).astype(bf16)
                y = jnp.dot(
                    probabilities,
                    jnp.where(inside, value[:, low:high], zero),
                    preferred_element_type=f32,
                )
                for s, (a, b) in enumerate(spans):
                    if low <= a and b <= high:
                        totals[s] = totals[s] + y[:, a - low : b - low]
            shifted = jnp.concatenate(
                [jnp.zeros((slot_rows, used - low_out), f32)] + totals, axis=-1
            )
            attended_ref[rows, :] = shifted.astype(bf16)
            return carry

        lax.fori_loop(0, per, one_slot, 0)

        def out_column(t, carry):
            at = pl.ds(pl.multiple_of(t * column, column), column)
            residual_ref[:, at] = residual_ref[:, at] + lax.dot_general(
                attended_ref[...],
                w_attention[group, at, low_out:total_width],
                (((1,), (1,)), ((), ())),
                preferred_element_type=f32,
            )
            return carry

        lax.fori_loop(0, depth // column, out_column, 0)
        return carry

    lax.fori_loop(0, groups, one_group, 0)

    norm_tile = tile_of(piece_rows, 32)
    for h in range(pieces):

        def norm_some(i, carry, h=h):
            rows = pl.ds(pl.multiple_of(i * norm_tile, norm_tile), norm_tile)
            at = pl.ds(pl.multiple_of(h * piece_rows + i * norm_tile, norm_tile), norm_tile)
            blocks[0, h, rows, :] = norm_rows(residual_ref[at, :], gain_ref[1:2], shift_ref[1:2])
            return carry

        lax.fori_loop(0, piece_rows // norm_tile, norm_some, 0)

    def out_copy(k, h):
        at = k * pieces + h
        return remote(blocks.at[0, h], blocks.at[k, h], send_a.at[at], recv_a.at[at], peer(k))

    def back_copy(k, h):
        at = k * pieces + h
        return remote(parts.at[k, h], backs.at[k, h], send_b.at[at], recv_b.at[at], peer(k))

    def forward(h):
        held, k = (1, 2) if h == 0 else (2, 1)
        at = 3 * pieces + h
        return remote(blocks.at[held, h], blocks.at[3, h], send_a.at[at], recv_a.at[at], peer(k))

    def across(h):
        at = 3 * pieces + h
        return remote(parts.at[3, h], relay.at[h], send_b.at[at], recv_b.at[at], peer(1 + h))

    for k, h in ((1, 0), (2, 1), (1, 1), (2, 0)):
        out_copy(k, h).start()
    mlp_held(1, 3)
    for j in range(2):
        for plane in range(planes):
            at = w_mlp.at[0, pl.ds(0, shard_rows), :]
            remote(
                at, at, mlp_twin.at[0], mlp_twin_recv.at[j * planes + plane], twin
            ).wait_recv()

    def mlp_step(i, carry):
        late = (i + 2) // 8
        middle = ((i + 2) // 4) % 2
        k = middle * (1 + i % 2) + 3 * late
        h = (i // 4 + i % 2) % 2

        @pl.when(i == 2)
        def _():
            out_copy(1, 0).wait_recv()
            forward(0).start()
            out_copy(2, 1).wait_recv()
            forward(1).start()

        @pl.when(i >= 4)
        def _():
            out_copy(k, h).wait_recv()

        def up(t, carry):
            at = pl.ds(pl.multiple_of(t * column, column), column)
            y = jnp.dot(blocks[k, h], w_mlp[0, :, at], preferred_element_type=f32) + b_up_ref[:, at]
            y = 0.5 * y * (1.0 + lax.erf(y * math.sqrt(0.5)))
            hidden_ref[:, at] = y.astype(bf16)
            return carry

        lax.fori_loop(0, hidden_ref.shape[1] // column, up, 0)

        def down(t, carry):
            at = pl.ds(pl.multiple_of(t * column, column), column)
            parts[k, h, :, at] = lax.dot_general(
                hidden_ref[...],
                w_mlp[1, at, :],
                (((1,), (1,)), ((), ())),
                preferred_element_type=f32,
            ).astype(bf16)
            return carry

        lax.fori_loop(0, depth // column, down, 0)

        @pl.when(i == 2)
        def _():
            back_copy(1, 0).start()

        @pl.when(i == 3)
        def _():
            back_copy(2, 1).start()

        @pl.when(i == 6)
        def _():
            across(1).start()

        @pl.when(i == 7)
        def _():
            across(0).start()

        return carry

    lax.fori_loop(0, 8, mlp_step, 0)
    for h, k in ((1, 1), (0, 2)):
        across(h).wait_recv()

        def add(i, carry, h=h, k=k):
            rows = pl.ds(pl.multiple_of(i * norm_tile, norm_tile), norm_tile)
            parts[k, h, rows, :] = (
                parts[k, h, rows, :].astype(f32) + relay[h, rows, :].astype(f32)
            ).astype(bf16)
            return carry

        lax.fori_loop(0, piece_rows // norm_tile, add, 0)
        back_copy(k, h).start()
    for k, h in ((1, 0), (2, 1), (1, 1), (2, 0)):
        back_copy(k, h).wait_recv()
    for h in range(pieces):

        def finish(i, carry, h=h):
            rows = pl.ds(pl.multiple_of(i * norm_tile, norm_tile), norm_tile)
            at = pl.ds(pl.multiple_of(h * piece_rows + i * norm_tile, norm_tile), norm_tile)
            total = residual_ref[at, :] + b_down_ref[...] + parts[0, h, rows, :].astype(f32)
            for k in (1, 2):
                total = total + backs[k, h, rows, :].astype(f32)
            live = label_col_ref[h, rows, :] >= 0
            out_ref[h, rows, :] = jnp.where(live, total, 0.0).astype(bf16)
            return carry

        lax.fori_loop(0, piece_rows // norm_tile, finish, 0)

    for h in range(2):
        forward(h).wait_send()
        across(h).wait_send()
        for k in (1, 2):
            out_copy(k, h).wait_send()
            back_copy(k, h).wait_send()
    for k in range(1, groups):
        bias_copy(k).wait_send()
    for g in range(groups):

        @pl.when(mp != g)
        def _():
            for i in range(half_images):
                token_copy(g, i).wait_send()

    def slot_sent(dest, carry):
        @pl.when(jnp.logical_not(jnp.logical_and(is_home, dest == dp)))
        def _():
            slot_copy(dest).wait_send()

        return carry

    lax.fori_loop(0, shards, slot_sent, 0)
    for p in range(planes):
        plane = arrival(p)

        @pl.when(jnp.logical_and(plane <= z, z < last))
        def _():
            att_copy(mp, plane, att_up.at[plane], above).wait_send()
            for j in range(2):
                mlp_copy(j, plane, mlp_up.at[j * planes + plane], above).wait_send()

        @pl.when(jnp.logical_and(plane >= z, z > 0))
        def _():
            att_copy(mp, plane, att_down.at[plane], below).wait_send()
            for j in range(2):
                mlp_copy(j, plane, mlp_down.at[j * planes + plane], below).wait_send()

        for g in range(groups):
            att_to_twin(g, plane).wait_send()
        for j in range(2):
            mlp_to_twin(j, plane).wait_send()
        for k in (1, 2):
            att_over(k, mp, plane, 0).wait_send()
        k = 1 + p % 2
        att_over(3 - k, flip(mp, k, groups), plane, 1).wait_send()


def layer_call(shards, groups, args, slot_rows):
    patches, keep, attention_shard, mlp_shard = args[0], args[2], args[8], args[11]
    images, _, depth = patches.shape
    keep_most = keep.shape[1]
    feature = depth // groups
    per = shards // groups
    rows = per * slot_rows
    planes = shards // 2
    half_images = images // 2
    vmem = pl.BlockSpec(memory_space=pltpu.VMEM)
    bf16 = jnp.bfloat16
    hidden = mlp_shard.shape[2]
    dma = pltpu.SemaphoreType.DMA
    buffer = pltpu.VMEM((groups, per, slot_rows, depth), bf16)
    used = 3 * feature
    return pl.pallas_call(
        functools.partial(layer_kernel, shards, groups),
        out_shape=jax.ShapeDtypeStruct((per, slot_rows, depth), bf16),
        in_specs=[pl.BlockSpec(memory_space=pl.ANY)] + [vmem] * (len(args) - 1),
        out_specs=vmem,
        scratch_shapes=[
            pltpu.VMEM(patches.shape, bf16),
            pltpu.VMEM((groups, half_images * keep_most, 2 * feature), bf16),
            pltpu.VMEM((groups, half_images * keep_most, 2 * feature), bf16),
            pltpu.VMEM((shards, slot_rows // 2, 2 * feature), bf16),
            pltpu.VMEM((shards, slot_rows // 2, 2 * feature), bf16),
            pltpu.VMEM((groups, shards * attention_shard.shape[0], attention_shard.shape[1]), bf16),
            pltpu.VMEM((groups,) + args[9].shape, jnp.float32),
            pltpu.VMEM((2, shards * mlp_shard.shape[1], hidden), bf16),
            pltpu.VMEM((rows, depth), bf16),
            pltpu.VMEM((rows, args[9].shape[1]), bf16),
            pltpu.VMEM((rows, attention_shard.shape[1] - used // 128 * 128), bf16),
            pltpu.VMEM((rows, depth), jnp.float32),
            buffer,
            buffer,
            buffer,
            pltpu.VMEM((per, slot_rows, depth), bf16),
            pltpu.VMEM((slot_rows, hidden), bf16),
            dma((images,)),
            dma((3,)),
            dma((groups * half_images,)),
            dma((groups * half_images,)),
            dma((shards,)),
            dma((shards,)),
            dma((groups,)),
            dma((groups,)),
            dma((planes,)),
            dma((planes,)),
            dma((6 * planes,)),
            dma((groups * planes,)),
            dma((groups * planes,)),
            dma((groups * planes,)),
            dma((2 * planes,)),
            dma((2 * planes,)),
            dma((2 * planes,)),
            dma((2 * planes,)),
            dma((2 * planes,)),
            dma((groups * per,)),
            dma((groups * per,)),
            dma((groups * per,)),
            dma((groups * per,)),
        ],
        compiler_params=pltpu.CompilerParams(
            collective_id=3, has_side_effects=True, vmem_limit_bytes=60 * 1024 * 1024
        ),
        cost_estimate=pl.CostEstimate(flops=100_000_000_000, bytes_accessed=0, transcendentals=0),
        name="layer",
    )(*args)


def one_kernel(
    patches,
    position,
    keep,
    counts,
    offsets,
    ln_gain,
    ln_bias,
    w_qkv,
    b_qkv,
    w_o,
    b_o,
    w_up,
    b_up,
    w_down,
    b_down,
):
    local_images, _, depth = patches.shape
    keep_most = keep.shape[1]
    shards = lax.axis_size("dp")
    groups = lax.axis_size("mp")
    images_here = local_images * groups
    slot_rows = slot_size(images_here, shards, keep_most)
    pack_rows = slot_rows * shards
    per = shards // groups
    dp = lax.axis_index("dp")
    mp = lax.axis_index("mp")
    feature = depth // groups

    own_counts = lax.dynamic_slice_in_dim(counts, dp * images_here, images_here)
    own_offsets = lax.dynamic_slice_in_dim(offsets, dp * images_here, images_here)
    shard = own_offsets // pack_rows
    base = shard * slot_rows + own_offsets - shard * pack_rows - dp * slot_rows
    step = jnp.arange(keep_most, dtype=jnp.int32)
    target = jnp.where(step[None, :] < own_counts[:, None], base[:, None] + step[None, :], -1)
    target = target.reshape(groups, 2, -1).transpose(1, 0, 2).reshape(2, 1, -1)

    first = dp * pack_rows + mp * per * slot_rows
    rows = first + jnp.arange(per * slot_rows, dtype=jnp.int32)
    inside = (rows[:, None] >= offsets[None, :]) & (rows[:, None] < (offsets + counts)[None, :])
    image_ids = jnp.arange(counts.shape[0], dtype=jnp.int32)
    labels = jnp.max(jnp.where(inside, image_ids[None, :] + 1, 0), axis=1) - 1
    labels = labels.reshape(per, slot_rows)

    attention_shard = jnp.concatenate([w_qkv[0, 0], w_qkv[0, 1], w_qkv[0, 2], w_o[0].T], axis=1)
    mlp_shard = jnp.stack([w_up[0], w_down[0].T])
    bias = b_qkv[0].reshape(1, -1)
    pad = (3 * feature + 255) // 256 * 256 - 3 * feature
    bias = jnp.broadcast_to(jnp.pad(bias, ((0, 0), (0, pad))), (8, 3 * feature + pad))
    return layer_call(
        shards,
        groups,
        (
            patches,
            position,
            keep[:, :, None],
            target,
            labels[:, :, None],
            labels[:, None, :],
            ln_gain[0],
            ln_bias[0],
            attention_shard,
            bias,
            b_o,
            mlp_shard,
            b_up,
            b_down,
        ),
        slot_rows,
    ).reshape(per * slot_rows, depth)


def solution(mesh):
    in_specs = (
        P(("dp", "mp"), None, None),
        P(),
        P(("dp", "mp"), None),
        P(),
        P(),
        P(),
        P(),
        P(None, None, "dp", "mp"),
        P(None, None, "mp"),
        P(None, "mp", "dp"),
        P(),
        P(None, "dp", "mp"),
        P(None, "mp"),
        P(None, "mp", "dp"),
        P(),
    )
    out_specs = P(("dp", "mp"), None)
    square = mesh.shape["mp"] == 4 and mesh.shape["dp"] == 8
    return jax.shard_map(
        one_kernel if square else per_device, mesh=mesh, in_specs=in_specs, out_specs=out_specs, check_vma=False
    )
```

```python
import functools
import math

import jax
import jax.numpy as jnp
from jax import lax
from jax.experimental import pallas as pl
from jax.experimental.pallas import tpu as pltpu
from jax.sharding import PartitionSpec as P

HEAD = 80
MESH = pl.DeviceIdType.MESH


def norm_rows(values, gain_row, shift_row):
    row_mean = jnp.mean(values, axis=-1, keepdims=True)
    centred = values - row_mean
    spread = jnp.mean(centred * centred, axis=-1, keepdims=True)
    return (centred * lax.rsqrt(spread + 1e-06) * gain_row + shift_row).astype(jnp.bfloat16)


def flip(index, mask, count):
    result = index
    bit = 1
    while bit < count:
        wanted = (mask // bit) % 2
        own = (index // bit) % 2
        result = result + bit * wanted * (1 - 2 * own)
        bit = bit * 2
    return result


def tile_of(extent, most):
    tile = most
    while extent % tile != 0:
        tile = tile // 2
    return tile


def route_kernel(
    shards,
    groups,
    packed_ref,
    gain_ref,
    shift_ref,
    stream_ref,
    normed_ref,
    out_ref,
    send_sem,
    recv_sem,
    own_sem,
):
    per = shards // groups
    dp = lax.axis_index("dp")
    mp = lax.axis_index("mp")
    home = dp // per
    slot = lax.rem(dp, per) * groups + mp

    barrier = pltpu.get_barrier_semaphore()
    for j in range(per):
        for g in range(groups):
            source = mp * per + j

            @pl.when(jnp.logical_or(source != dp, mp != g))
            def _():
                pl.semaphore_signal(barrier, inc=1, device_id=(source, g), device_id_type=MESH)

    is_home = home == mp

    @pl.when(is_home)
    def _():
        pl.semaphore_wait(barrier, shards - 1)

    @pl.when(jnp.logical_not(is_home))
    def _():
        pl.semaphore_wait(barrier, shards)

    def remote(step):
        dest = lax.rem(dp + step, shards)
        return pltpu.make_async_remote_copy(
            src_ref=packed_ref.at[dest],
            dst_ref=out_ref.at[slot],
            send_sem=send_sem.at[step],
            recv_sem=recv_sem.at[slot],
            device_id=(dest, home),
            device_id_type=MESH,
        )

    own = pltpu.make_async_copy(packed_ref.at[dp], out_ref.at[slot], own_sem)
    for step in range(1, shards):
        remote(step).start()

    @pl.when(is_home)
    def _():
        own.start()
        own.wait()

    @pl.when(jnp.logical_not(is_home))
    def _():
        remote(0).start()
        remote(0).wait_send()

    for step in range(1, shards):
        remote(step).wait_send()
    for j in range(per):
        for g in range(groups):
            source = mp * per + j

            @pl.when(jnp.logical_or(source != dp, mp != g))
            def _():
                pltpu.make_async_remote_copy(
                    src_ref=packed_ref.at[0],
                    dst_ref=out_ref.at[j * groups + g],
                    send_sem=send_sem.at[0],
                    recv_sem=recv_sem.at[j * groups + g],
                    device_id=(dp, mp),
                    device_id_type=MESH,
                ).wait_recv()

    rows_tile = tile_of(packed_ref.shape[1], 32)
    for j in range(per):

        def some(i, carry):
            rows = pl.ds(pl.multiple_of(i * rows_tile, rows_tile), rows_tile)
            whole = jnp.concatenate(
                [out_ref[j * groups + g, rows, :] for g in range(groups)], axis=-1
            )
            stream_ref[j, rows, :] = whole
            normed_ref[j, rows, :] = norm_rows(
                whole.astype(jnp.float32), gain_ref[...], shift_ref[...]
            )
            return carry

        lax.fori_loop(0, packed_ref.shape[1] // rows_tile, some, 0)


def route(packed, gain_row, shift_row, shards, groups):
    slot_rows, width = packed.shape[1:]
    result = jax.ShapeDtypeStruct((shards // groups, slot_rows, width * groups), packed.dtype)
    vmem = pl.BlockSpec(memory_space=pltpu.VMEM)
    return pl.pallas_call(
        functools.partial(route_kernel, shards, groups),
        out_shape=(result, result),
        in_specs=[vmem] * 3,
        out_specs=(vmem, vmem),
        scratch_shapes=[
            pltpu.VMEM(packed.shape, packed.dtype),
            pltpu.SemaphoreType.DMA((shards,)),
            pltpu.SemaphoreType.DMA((shards,)),
            pltpu.SemaphoreType.DMA,
        ],
        compiler_params=pltpu.CompilerParams(collective_id=0, has_side_effects=True),
        cost_estimate=pl.CostEstimate(flops=15_000_000_000, bytes_accessed=0, transcendentals=0),
        name="route",
    )(packed, gain_row, shift_row)


def exchange(groups, x_ref, blocks, parts, backs, relay, sems, block_step, finish):
    own_sem, send_a, recv_a, send_b, recv_b = sems
    dp = lax.axis_index("dp")
    mp = lax.axis_index("mp")
    pieces = x_ref.shape[0]
    square = groups == 4 and pieces == 2
    partners = range(1, 3) if square else range(1, groups)

    barrier = pltpu.get_barrier_semaphore()
    for k in partners:
        pl.semaphore_signal(
            barrier, inc=1, device_id=(dp, flip(mp, k, groups)), device_id_type=MESH
        )
    own = pltpu.make_async_copy(x_ref, blocks.at[pl.ds(0, pieces)], own_sem)
    own.start()
    pl.semaphore_wait(barrier, len(partners))

    def send(source, target, out_sem, in_sem, k):
        return pltpu.make_async_remote_copy(
            src_ref=source,
            dst_ref=target,
            send_sem=out_sem,
            recv_sem=in_sem,
            device_id=(dp, flip(mp, k, groups)),
            device_id_type=MESH,
        )

    def out_copy(k, h):
        at = k * pieces + h
        return send(x_ref.at[h], blocks.at[at], send_a.at[at], recv_a.at[at], k)

    def back_copy(k, h):
        at = k * pieces + h
        return send(parts.at[at], backs.at[at], send_b.at[at], recv_b.at[at], k)

    if square:
        def forward(h):
            held, k = (2, 2) if h == 0 else (5, 1)
            at = 6 + h
            return send(blocks.at[held], blocks.at[at], send_a.at[at], recv_a.at[at], k)

        def across(h):
            at = 6 + h
            return send(parts.at[at], relay.at[h], send_b.at[at], recv_b.at[at], 1 + h)

        for k, h in ((1, 0), (2, 1), (1, 1), (2, 0)):
            out_copy(k, h).start()
        own.wait()

        def step(i, carry):
            late = (i + 2) // 8
            middle = ((i + 2) // 4) % 2
            k = middle * (1 + i % 2) + 3 * late
            h = (i // 4 + i % 2) % 2

            @pl.when(i == 2)
            def _():
                out_copy(1, 0).wait_recv()
                forward(0).start()
                out_copy(2, 1).wait_recv()
                forward(1).start()

            @pl.when(i >= 4)
            def _():
                out_copy(k, h).wait_recv()

            block_step(k * 2 + h, flip(mp, k, groups) * 2 + h)

            @pl.when(i == 2)
            def _():
                back_copy(1, 0).start()

            @pl.when(i == 3)
            def _():
                back_copy(2, 1).start()

            @pl.when(i == 6)
            def _():
                across(1).start()

            @pl.when(i == 7)
            def _():
                across(0).start()

            return carry

        lax.fori_loop(0, 8, step, 0)
        rows_tile = tile_of(x_ref.shape[1], 32)
        for h, k in ((1, 1), (0, 2)):
            across(h).wait_recv()

            def add(i, carry, h=h, k=k):
                rows = pl.ds(pl.multiple_of(i * rows_tile, rows_tile), rows_tile)
                parts[k * 2 + h, rows, :] = (
                    parts[k * 2 + h, rows, :].astype(jnp.float32)
                    + relay[h, rows, :].astype(jnp.float32)
                ).astype(jnp.bfloat16)
                return carry

            lax.fori_loop(0, x_ref.shape[1] // rows_tile, add, 0)
            back_copy(k, h).start()
        for k, h in ((1, 0), (2, 1), (1, 1), (2, 0)):
            back_copy(k, h).wait_recv()
        finish(partners)
        for h in range(2):
            forward(h).wait_send()
            across(h).wait_send()
            for k in partners:
                out_copy(k, h).wait_send()
                back_copy(k, h).wait_send()
        return

    for k in partners:
        for h in range(pieces):
            out_copy(k, h).start()
    own.wait()

    def step(i, carry):
        k = i // pieces
        h = i % pieces

        @pl.when(k > 0)
        def _():
            out_copy(k, h).wait_recv()

        block_step(i, flip(mp, k, groups) * pieces + h)

        @pl.when(k > 0)
        def _():
            back_copy(k, h).start()

        return carry

    lax.fori_loop(0, groups * pieces, step, 0)
    for k in partners:
        for h in range(pieces):
            back_copy(k, h).wait_recv()
    finish(partners)
    for k in partners:
        for h in range(pieces):
            out_copy(k, h).wait_send()
            back_copy(k, h).wait_send()


def finish_rows(x_ref, parts, backs, partners, write):
    pieces, row_count = x_ref.shape[:2]
    rows_tile = tile_of(row_count, 32)
    for h in range(pieces):

        def some(i, carry, h=h):
            rows = pl.ds(pl.multiple_of(i * rows_tile, rows_tile), rows_tile)
            total = parts[h, rows, :].astype(jnp.float32)
            for k in partners:
                total = total + backs[k * pieces + h, rows, :].astype(jnp.float32)
            write(h, rows, total)
            return carry

        lax.fori_loop(0, row_count // rows_tile, some, 0)


def attention_kernel(
    groups,
    x_ref,
    stream_ref,
    w_ref,
    b_ref,
    label_col_ref,
    label_row_ref,
    bias_ref,
    gain_ref,
    shift_ref,
    residual_ref,
    normed_ref,
    blocks,
    parts,
    backs,
    relay,
    attended_ref,
    *sems,
):
    row_count, depth = x_ref.shape[1:]
    width = w_ref.shape[2]
    heads = width // HEAD
    scale = 1.0 / math.sqrt(HEAD)
    tile = tile_of(depth, 256)

    def block_step(at_block, source):
        x = blocks[at_block]

        def project(t):
            y = jnp.dot(x, w_ref[t], preferred_element_type=jnp.float32)
            return (y + b_ref[t]).astype(jnp.bfloat16)

        query, key, value = project(0), project(1), project(2)
        matches = label_col_ref[source] == label_row_ref[source]
        lane_head = lax.broadcasted_iota(jnp.int32, (row_count, width), 1)
        total = jnp.zeros((row_count, width), jnp.float32)
        zero = jnp.zeros((row_count, width), jnp.bfloat16)
        for h in range(heads):
            inside = (lane_head >= h * HEAD) & (lane_head < (h + 1) * HEAD)
            scores = lax.dot_general(
                jnp.where(inside, query, zero),
                key,
                (((1,), (1,)), ((), ())),
                preferred_element_type=jnp.float32,
            )
            scores = jnp.where(matches, scores * scale, -jnp.inf)
            weights = jnp.exp(scores - jnp.max(scores, axis=-1, keepdims=True))
            inverse = 1.0 / jnp.sum(weights, axis=-1, keepdims=True)
            probabilities = (weights * inverse).astype(jnp.bfloat16)
            total = total + jnp.dot(
                probabilities, jnp.where(inside, value, zero), preferred_element_type=jnp.float32
            )
        attended_ref[...] = total.astype(jnp.bfloat16)

        def column(t, carry):
            at = pl.ds(pl.multiple_of(t * tile, tile), tile)
            parts[at_block, :, at] = lax.dot_general(
                attended_ref[...],
                w_ref[3, at, :],
                (((1,), (1,)), ((), ())),
                preferred_element_type=jnp.float32,
            ).astype(jnp.bfloat16)
            return carry

        lax.fori_loop(0, depth // tile, column, 0)

    def finish(partners):
        def write(h, rows, total):
            residual = stream_ref[h, rows, :].astype(jnp.float32) + total + bias_ref[...]
            residual_ref[h, rows, :] = residual
            normed_ref[h, rows, :] = norm_rows(residual, gain_ref[...], shift_ref[...])

        finish_rows(x_ref, parts, backs, partners, write)

    exchange(groups, x_ref, blocks, parts, backs, relay, sems, block_step, finish)


def mlp_kernel(
    groups,
    x_ref,
    residual_ref,
    up_ref,
    b_ref,
    down_ref,
    bias_ref,
    out_ref,
    blocks,
    parts,
    backs,
    relay,
    hidden_ref,
    *sems,
):
    row_count, depth = x_ref.shape[1:]
    width = up_ref.shape[1]
    tile = tile_of(depth, 256)
    up_tile = tile_of(width, 256)

    def block_step(at_block, source):
        def up(t, carry):
            at = pl.ds(pl.multiple_of(t * up_tile, up_tile), up_tile)
            y = jnp.dot(blocks[at_block], up_ref[:, at], preferred_element_type=jnp.float32) + b_ref[:, at]
            y = 0.5 * y * (1.0 + lax.erf(y * math.sqrt(0.5)))
            hidden_ref[:, at] = y.astype(jnp.bfloat16)
            return carry

        lax.fori_loop(0, width // up_tile, up, 0)

        def column(t, carry):
            at = pl.ds(pl.multiple_of(t * tile, tile), tile)
            parts[at_block, :, at] = lax.dot_general(
                hidden_ref[...],
                down_ref[at, :],
                (((1,), (1,)), ((), ())),
                preferred_element_type=jnp.float32,
            ).astype(jnp.bfloat16)
            return carry

        lax.fori_loop(0, depth // tile, column, 0)

    def finish(partners):
        def write(h, rows, total):
            out_ref[h, rows, :] = (residual_ref[h, rows, :] + total + bias_ref[...]).astype(
                jnp.bfloat16
            )

        finish_rows(x_ref, parts, backs, partners, write)

    exchange(groups, x_ref, blocks, parts, backs, relay, sems, block_step, finish)


def exchange_call(kernel, groups, args, outs, width, collective_id, name):
    pieces, row_count, depth = args[0].shape
    vmem = pl.BlockSpec(memory_space=pltpu.VMEM)
    many = pltpu.SemaphoreType.DMA((groups * pieces,))
    buffer = pltpu.VMEM((groups * pieces, row_count, depth), jnp.bfloat16)
    return pl.pallas_call(
        functools.partial(kernel, groups),
        out_shape=outs,
        in_specs=[vmem] * len(args),
        out_specs=jax.tree.map(lambda _: vmem, outs),
        scratch_shapes=[
            buffer,
            buffer,
            buffer,
            pltpu.VMEM((pieces, row_count, depth), jnp.bfloat16),
            pltpu.VMEM((row_count, width), jnp.bfloat16),
            pltpu.SemaphoreType.DMA,
            many,
            many,
            many,
            many,
        ],
        compiler_params=pltpu.CompilerParams(
            collective_id=collective_id, has_side_effects=True, vmem_limit_bytes=48 * 1024 * 1024
        ),
        cost_estimate=pl.CostEstimate(flops=50_000_000_000, bytes_accessed=0, transcendentals=0),
        name=name,
    )(*args)

def slot_size(images_here, shards, keep_most):
    per_slot = (images_here + shards - 1) // shards
    return max(keep_most + 16, per_slot * keep_most * 5 // 8)


def per_device(
    patches,
    position,
    keep,
    counts,
    offsets,
    ln_gain,
    ln_bias,
    w_qkv,
    b_qkv,
    w_o,
    b_o,
    w_up,
    b_up,
    w_down,
    b_down,
):
    local_images, patch_count, column_count = patches.shape
    keep_most = keep.shape[1]
    shard_count = lax.axis_size("dp")
    group_size = lax.axis_size("mp")
    images_here = local_images * group_size
    slot_rows = slot_size(images_here, shard_count, keep_most)
    pack_rows = slot_rows * shard_count
    local_rows = pack_rows // group_size
    dp_index = lax.axis_index("dp")
    mp_index = lax.axis_index("mp")
    f32 = jnp.float32

    attention_shard = jnp.concatenate([w_qkv[0], w_o[0].T[None]], axis=0)
    w_attention = lax.all_gather(attention_shard, "dp", axis=1, tiled=True)

    chosen = (keep[:, :, None] == jnp.arange(patch_count, dtype=jnp.int32)).astype(jnp.bfloat16)
    tokens = (
        jnp.einsum("ijp,ipd->ijd", chosen, patches, preferred_element_type=f32)
        + jnp.einsum("ijp,pd->ijd", chosen, position, preferred_element_type=f32)
    ).astype(jnp.bfloat16)
    tokens, w_up_shard = lax.optimization_barrier((tokens, w_up[0]))
    w_up_full = lax.all_gather(w_up_shard, "dp", axis=0, tiled=True)

    first_image = dp_index * images_here
    group_counts = lax.dynamic_slice_in_dim(counts, first_image, images_here)
    group_offsets = lax.dynamic_slice_in_dim(offsets, first_image, images_here)
    positions_in = jnp.arange(keep_most, dtype=jnp.int32)
    group_live = positions_in[None, :] < group_counts[:, None]
    shard_index = group_offsets // pack_rows
    base_row = (
        shard_index * slot_rows + group_offsets - shard_index * pack_rows - dp_index * slot_rows
    )
    target = jnp.where(group_live, base_row[:, None] + positions_in[None, :], pack_rows).reshape(-1)
    image_ids = jnp.arange(counts.shape[0], dtype=jnp.int32)
    packed_rows = dp_index * pack_rows + jnp.arange(pack_rows, dtype=jnp.int32)
    inside = (packed_rows[:, None] >= offsets[None, :]) & (
        packed_rows[:, None] < (offsets + counts)[None, :]
    )
    labels = jnp.max(jnp.where(inside, image_ids[None, :] + 1, 0), axis=1) - 1

    featured = lax.all_to_all(
        tokens.reshape(-1, column_count), "mp", split_axis=1, concat_axis=0, tiled=True
    )
    featured, w_down_shard = lax.optimization_barrier((featured, w_down[0]))
    w_down_rows = lax.all_gather(w_down_shard, "dp", axis=1, tiled=True).T
    feature_count = featured.shape[1]
    placing = (jnp.arange(pack_rows, dtype=jnp.int32)[:, None] == target[None, :]).astype(
        jnp.bfloat16
    )
    packed = jnp.dot(placing, featured, preferred_element_type=f32).astype(jnp.bfloat16)
    stream, normed = route(
        packed.reshape(shard_count, slot_rows, feature_count),
        ln_gain[:, 0],
        ln_bias[:, 0],
        shard_count,
        group_size,
    )
    pieces = stream.shape[0]
    by_piece = labels.reshape(group_size * pieces, local_rows // pieces)
    residual, normed_mlp = exchange_call(
        attention_kernel,
        group_size,
        (
            normed,
            stream,
            w_attention,
            b_qkv[0][:, None, :],
            by_piece[:, :, None],
            by_piece[:, None, :],
            b_o,
            ln_gain[:, 1],
            ln_bias[:, 1],
        ),
        (
            jax.ShapeDtypeStruct(stream.shape, f32),
            jax.ShapeDtypeStruct(stream.shape, jnp.bfloat16),
        ),
        w_attention.shape[2],
        1,
        "attention",
    )
    stream = exchange_call(
        mlp_kernel,
        group_size,
        (normed_mlp, residual, w_up_full, b_up, w_down_rows, b_down),
        jax.ShapeDtypeStruct(stream.shape, jnp.bfloat16),
        w_up_full.shape[1],
        2,
        "mlp",
    ).reshape(local_rows, column_count)
    own_labels = lax.dynamic_slice_in_dim(labels, mp_index * local_rows, local_rows)
    return jnp.where(own_labels[:, None] >= 0, stream, jnp.zeros_like(stream))

def by_pair(index, values):
    low = index % 2
    high = index // 2
    return (
        values[0] * (1 - low) * (1 - high)
        + values[1] * low * (1 - high)
        + values[2] * (1 - low) * high
        + values[3] * low * high
    )


ARRIVALS = ((0, 1, 2, 3), (1, 0, 2, 3), (2, 1, 3, 0), (3, 2, 1, 0))


def layer_kernel(
    shards,
    groups,
    patches_ref,
    position_ref,
    keep_ref,
    counts_ref,
    offsets_ref,
    gain_ref,
    shift_ref,
    w_qkv_ref,
    b_qkv_ref,
    w_o_ref,
    b_o_ref,
    w_up_ref,
    b_up_ref,
    w_down_ref,
    b_down_ref,
    out_ref,
    patch_buf,
    token_out,
    token_in,
    slot_out,
    slot_in,
    w_attention,
    b_attention,
    w_mlp,
    label_col,
    label_row,
    target,
    normed_ref,
    projected_ref,
    attended_ref,
    residual_ref,
    blocks,
    parts,
    backs,
    relay,
    hidden_ref,
    patch_sem,
    local_sem,
    token_send,
    token_recv,
    slot_send,
    slot_recv,
    bias_send,
    bias_recv,
    att_line,
    att_plane,
    att_twin,
    att_recv,
    att_twin_recv,
    mlp_line,
    mlp_twin,
    mlp_recv,
    mlp_twin_recv,
    send_a,
    recv_a,
    send_b,
    recv_b,
):
    f32 = jnp.float32
    bf16 = jnp.bfloat16
    dp = lax.axis_index("dp")
    mp = lax.axis_index("mp")
    per = shards // groups
    planes = shards // 2
    z = dp // 2
    core = dp % 2
    home = dp // per
    images, patch_count, depth = patches_ref.shape
    keep_most = keep_ref.shape[1]
    feature = depth // groups
    pieces, piece_rows = blocks.shape[1:3]
    shard_rows = w_up_ref.shape[0]
    half_images = images // 2
    last = planes - 1

    def remote(source, target, out_sem, in_sem, device):
        return pltpu.make_async_remote_copy(
            src_ref=source,
            dst_ref=target,
            send_sem=out_sem,
            recv_sem=in_sem,
            device_id=device,
            device_id_type=MESH,
        )

    def peer(k):
        return (dp, flip(mp, k, groups))

    twin = (dp + 1 - 2 * core, mp)

    def along(distance):
        return (lax.rem(dp + 2 * distance + shards, shards), mp)

    for i in range(images):
        pltpu.make_async_copy(patches_ref.at[i], patch_buf.at[i], patch_sem.at[i]).start()

    barrier = pltpu.get_barrier_semaphore()
    for j in range(per):
        for g in range(groups):
            source = mp * per + j

            @pl.when(jnp.logical_or(source != dp, mp != g))
            def _():
                pl.semaphore_signal(barrier, inc=1, device_id=(source, g), device_id_type=MESH)

    for k in range(1, groups):
        pl.semaphore_signal(barrier, inc=1, device_id=peer(k), device_id_type=MESH)
    pl.semaphore_signal(barrier, inc=1, device_id=twin, device_id_type=MESH)

    for distance in (-2, -1, 1, 2):

        @pl.when(jnp.logical_and(z + distance >= 0, z + distance <= last))
        def _():
            pl.semaphore_signal(barrier, inc=1, device_id=along(distance), device_id_type=MESH)

    own_rows = pl.ds(pl.multiple_of(dp * shard_rows, 16), shard_rows)
    own_up = pltpu.make_async_copy(w_up_ref, w_mlp.at[0, own_rows, :], local_sem.at[0])
    own_up.start()
    for t in range(3):
        at = slice(t * feature, (t + 1) * feature)
        b_attention[mp, :, at] = jnp.broadcast_to(b_qkv_ref[t : t + 1, :], (8, feature))
        w_attention[mp, own_rows, at] = w_qkv_ref[t]
    w_attention[mp, own_rows, 3 * feature :] = jnp.transpose(w_o_ref[...])
    is_home = home == mp
    away = jnp.where(is_home, 0, 1)
    between = jnp.where(jnp.logical_and(z > 0, z < last), 1, 0)
    pl.semaphore_wait(barrier, shards + groups + 1 + away + between)

    own_up.wait()
    edge_plane = jnp.logical_or(z == 0, z == last)

    def rows_of(plane):
        return pl.ds(pl.multiple_of((2 * plane + core) * shard_rows, 16), shard_rows)

    def att_copy(group, plane, out_sem, device):
        at = w_attention.at[group, rows_of(plane), :]
        return remote(at, at, out_sem, att_recv.at[group * planes + plane], device)

    def att_to_twin(group, plane):
        at = w_attention.at[group, rows_of(plane), :]
        index = group * planes + plane
        return remote(at, at, att_twin.at[index], att_twin_recv.at[index], twin)

    def att_over(k, group, plane, relayed):
        return att_copy(group, plane, att_plane.at[(k * 2 + relayed) * planes + plane], peer(k))

    def arrival(p):
        return by_pair(z, [row[p] for row in ARRIVALS])

    def to_line(index, at, out_sems, in_sem, act):
        for way, distance in enumerate((1, -1, 2, -2)):

            @pl.when(jnp.logical_and(z + distance >= 0, z + distance <= last))
            def _():
                copy = remote(at, at, out_sems.at[4 * index + way], in_sem, along(distance))
                if act:
                    copy.start()
                else:
                    copy.wait_send()

    def to_end(index, at, out_sems, in_sem, act):
        for way, at_plane, distance in ((1, 1, -1), (0, last - 1, 1)):

            @pl.when(z == at_plane)
            def _():
                copy = remote(at, at, out_sems.at[4 * index + way], in_sem, along(distance))
                if act:
                    copy.start()
                else:
                    copy.wait_send()

    def att_own(act):
        at = w_attention.at[mp, rows_of(z), :]
        to_line(0, at, att_line, att_recv.at[mp * planes + z], act)

    def att_end(act):
        plane = arrival(last)
        at = w_attention.at[mp, rows_of(plane), :]
        to_end(1, at, att_line, att_recv.at[mp * planes + plane], act)

    def att_held(p):
        plane = arrival(p)
        if p > 0:
            att_copy(mp, plane, att_twin.at[0], twin).wait_recv()
        else:
            att_own(True)
        if p == last:
            att_end(True)
        att_to_twin(mp, plane).start()

    def att_spread(p):
        plane = arrival(p)
        for k in (1, 2):
            att_over(k, mp, plane, 0).start()

    def att_near(p):
        plane = arrival(p)
        for k in (1, 2):
            group = flip(mp, k, groups)
            att_copy(group, plane, att_twin.at[0], twin).wait_recv()
            if p % 2 == k - 1:
                att_over(3 - k, group, plane, 1).start()
            att_to_twin(group, plane).start()

    def att_far(p):
        plane = arrival(p)
        group = flip(mp, 3, groups)
        att_copy(group, plane, att_twin.at[0], twin).wait_recv()
        att_to_twin(group, plane).start()

    def mlp_copy(j, plane, out_sem, device):
        at = w_mlp.at[j, rows_of(plane), :]
        return remote(at, at, out_sem, mlp_recv.at[j * planes + plane], device)

    def mlp_to_twin(j, plane):
        at = w_mlp.at[j, rows_of(plane), :]
        index = j * planes + plane
        return remote(at, at, mlp_twin.at[index], mlp_twin_recv.at[index], twin)

    def mlp_own(j, act):
        at = w_mlp.at[j, rows_of(z), :]
        to_line(2 * j, at, mlp_line, mlp_recv.at[j * planes + z], act)

    def mlp_end(j, act):
        plane = arrival(last)
        at = w_mlp.at[j, rows_of(plane), :]
        to_end(2 * j + 1, at, mlp_line, mlp_recv.at[j * planes + plane], act)

    def mlp_held(j, p):
        plane = arrival(p)
        if p > 0:
            mlp_copy(j, plane, mlp_twin.at[0], twin).wait_recv()
        else:
            mlp_own(j, True)
        if p == last:
            mlp_end(j, True)
        mlp_to_twin(j, plane).start()

    def bias_copy(k):
        return remote(
            b_attention.at[mp], b_attention.at[mp], bias_send.at[k], bias_recv.at[mp], peer(k)
        )

    for k in range(1, groups):
        bias_copy(k).start()
    att_held(0)

    def token_copy(g, i):
        rows = pl.ds(pl.multiple_of(i * keep_most, keep_most), keep_most)
        return remote(
            token_out.at[g, rows, :],
            token_in.at[mp, rows, :],
            token_send.at[g * half_images + i],
            token_recv.at[mp * half_images + i],
            (dp, g),
        )

    def own_tokens(i):
        rows = pl.ds(pl.multiple_of(i * keep_most, keep_most), keep_most)
        return pltpu.make_async_copy(
            token_out.at[mp, rows, :],
            token_in.at[mp, rows, :],
            token_recv.at[mp * half_images + i],
        )

    patch_ids = lax.broadcasted_iota(jnp.int32, (patch_count, keep_most), 0)

    def pick(i):
        pltpu.make_async_copy(patches_ref.at[i], patch_buf.at[i], patch_sem.at[i]).wait()
        chosen = (keep_ref[pl.ds(i, 1), :] == patch_ids).astype(bf16)
        dims = (((0,), (0,)), ((), ()))
        return lax.dot_general(
            chosen, patch_buf[i], dims, preferred_element_type=f32
        ) + lax.dot_general(chosen, position_ref[...], dims, preferred_element_type=f32)

    def some_tokens(i, carry):
        rows = pl.ds(pl.multiple_of(i * keep_most, keep_most), keep_most)
        left = pick(i)
        right = pick(i + half_images)
        for g in range(groups):
            at = slice(g * feature, (g + 1) * feature)
            token_out[g, rows, :] = jnp.concatenate([left[:, at], right[:, at]], axis=-1).astype(
                bf16
            )
        for g in range(groups):

            @pl.when(mp != g)
            def _():
                token_copy(g, i).start()

        own_tokens(i).start()
        return carry

    lax.fori_loop(0, half_images, some_tokens, 0)
    att_spread(0)

    slot_rows = 2 * slot_out.shape[1]
    half_rows = slot_out.shape[1]
    images_here = images * groups
    token_count = groups * half_images * keep_most
    lane = lax.broadcasted_iota(jnp.int32, (1, token_count), 1)
    lane_image = lane // keep_most
    lane_step = lane % keep_most
    pack_rows = shards * slot_rows
    for half in range(2):

        def aim(q, row, half=half):
            image = dp * images_here + (q // half_images) * images + half * half_images
            image = image + q % half_images
            offset = offsets_ref[image]
            live = jnp.logical_and(lane_image == q, lane_step < counts_ref[image])
            return jnp.where(live, offset + lane_step, row)

        row = lax.fori_loop(
            0, groups * half_images, aim, jnp.full((1, token_count), -1, jnp.int32)
        )
        target[half] = row

    for j in range(per):
        first = dp * pack_rows + (mp * per + j) * slot_rows
        row_at = first + lax.broadcasted_iota(jnp.int32, (1, slot_rows), 1)
        col_at = first + lax.broadcasted_iota(jnp.int32, (slot_rows, 128), 0)

        def tell(q, found, j=j, row_at=row_at, col_at=col_at):
            in_row, in_col = found
            image = (mp * per + j) * images_here + q
            low = offsets_ref[image]
            high = low + counts_ref[image]
            in_row = jnp.where(jnp.logical_and(row_at >= low, row_at < high), image, in_row)
            in_col = jnp.where(jnp.logical_and(col_at >= low, col_at < high), image, in_col)
            return in_row, in_col

        none = (
            jnp.full((1, slot_rows), -1, jnp.int32),
            jnp.full((slot_rows, 128), -1, jnp.int32),
        )
        in_row, in_col = lax.fori_loop(0, images_here, tell, none)
        label_row[j] = in_row
        label_col[j] = in_col

    w_mlp[1, own_rows, :] = jnp.transpose(w_down_ref[...])
    att_held(1)
    att_spread(1)

    def tokens_here(k, carry):
        group = flip(mp, k, groups)

        def one(i, carry):
            remote(
                token_out.at[0, pl.ds(0, keep_most), :],
                token_in.at[group, pl.ds(pl.multiple_of(i * keep_most, keep_most), keep_most), :],
                token_send.at[0],
                token_recv.at[group * half_images + i],
                twin,
            ).wait_recv()
            return carry

        return lax.fori_loop(0, half_images, one, carry)

    for i in range(half_images):
        own_tokens(i).wait()
    lax.fori_loop(1, groups, tokens_here, 0)

    def slot_copy(dest):
        slot = lax.rem(dp, per) * groups + mp
        return remote(
            slot_out.at[dest],
            slot_in.at[slot],
            slot_send.at[dest],
            slot_recv.at[slot],
            (dest, home),
        )

    def own_slot():
        slot = lax.rem(dp, per) * groups + mp
        return pltpu.make_async_copy(slot_out.at[dp], slot_in.at[slot], slot_recv.at[slot])

    edge = feature // 128 * 128
    width = feature - edge + feature

    def place(i, carry):
        row = lax.broadcasted_iota(jnp.int32, (2 * slot_rows, token_count), 0)
        below = row < slot_rows
        first = 2 * i * pack_rows + dp * slot_rows
        rows = row + jnp.where(below, first, first + pack_rows - slot_rows)
        left = (rows == target[0]).astype(bf16)
        right = (rows == target[1]).astype(bf16)
        tokens = token_in[...].reshape(token_count, 2 * feature)
        whole = (
            jnp.dot(left, tokens[:, :width], preferred_element_type=f32)[:, :feature]
            + jnp.dot(right, tokens[:, edge:], preferred_element_type=f32)[:, feature - edge :]
        )
        for j in range(2):
            upper = whole[2 * j * half_rows : (2 * j + 1) * half_rows]
            lower = whole[(2 * j + 1) * half_rows : (2 * j + 2) * half_rows]
            slot_out[2 * i + j] = jnp.concatenate([upper, lower], axis=-1).astype(bf16)
        for j in range(2):
            dest = 2 * i + j
            stays = jnp.logical_and(is_home, dest == dp)

            @pl.when(stays)
            def _():
                own_slot().start()

            @pl.when(jnp.logical_not(stays))
            def _():
                slot_copy(dest).start()

        return carry

    lax.fori_loop(0, shards // 2, place, 0)
    att_held(2)
    att_spread(2)

    @pl.when(jnp.logical_not(edge_plane))
    def _():
        att_held(3)
        att_spread(3)

    mlp_held(0, 0)
    att_near(0)

    @pl.when(edge_plane)
    def _():
        att_held(3)
        att_spread(3)

    att_near(1)

    for j in range(per):
        for g in range(groups):
            source = mp * per + j
            stays = jnp.logical_and(source == dp, mp == g)

            @pl.when(stays)
            def _():
                own_slot().wait()

            @pl.when(jnp.logical_not(stays))
            def _():
                remote(
                    slot_out.at[0],
                    slot_in.at[j * groups + g],
                    slot_send.at[0],
                    slot_recv.at[j * groups + g],
                    twin,
                ).wait_recv()

    rows_tile = tile_of(half_rows, 16)
    steps = half_rows // rows_tile

    def assemble(i, carry):
        j = i // (2 * steps)
        half = (i // steps) % 2
        rows = pl.ds(pl.multiple_of((i % steps) * rows_tile, rows_tile), rows_tile)

        def put(low):
            whole = jnp.concatenate(
                [
                    slot_in[j * groups + g, rows, :][:, low : low + feature]
                    for g in range(groups)
                ],
                axis=-1,
            ).astype(f32)
            to = pl.ds(pl.multiple_of(i * rows_tile, rows_tile), rows_tile)
            residual_ref[to, :] = whole + b_o_ref[...]
            normed_ref[to, :] = norm_rows(whole, gain_ref[0:1], shift_ref[0:1])

        @pl.when(half == 0)
        def _():
            put(0)

        @pl.when(half == 1)
        def _():
            put(feature)

        return carry

    lax.fori_loop(0, 2 * per * steps, assemble, 0)
    att_near(2)

    heads = feature // HEAD
    scale = 1.0 / math.sqrt(HEAD)
    used = 3 * feature
    total_width = w_attention.shape[2]
    column = 256
    low_out = used // 128 * 128
    low_key = feature // 128 * 128

    def one_group(step, carry):
        group = flip(mp, step, groups)

        @pl.when(step == 1)
        def _():
            mlp_held(0, 1)
            att_near(3)
            mlp_held(1, 0)
            mlp_held(0, 2)
            att_far(0)
            att_far(1)

        @pl.when(jnp.logical_and(step == 2, jnp.logical_not(edge_plane)))
        def _():
            mlp_held(0, 3)

        @pl.when(step == 3)
        def _():
            att_far(2)
            att_far(3)
            mlp_held(1, 1)

        @pl.when(step > 0)
        def _():
            remote(
                b_attention.at[0], b_attention.at[group], bias_send.at[0], bias_recv.at[group], twin
            ).wait_recv()

        for plane in range(planes):
            at = w_attention.at[group, pl.ds(0, shard_rows), :]
            remote(
                at, at, att_twin.at[0], att_twin_recv.at[group * planes + plane], twin
            ).wait_recv()

        def project(t, carry):
            at = pl.ds(pl.multiple_of(t * column, column), column)
            y = jnp.dot(normed_ref[...], w_attention[group, :, at], preferred_element_type=f32)
            projected_ref[:, at] = (y + b_attention[group, 0:1, at]).astype(bf16)
            return carry

        lax.fori_loop(0, projected_ref.shape[1] // column, project, 0)

        def one_slot(j, carry):
            rows = pl.ds(pl.multiple_of(j * slot_rows, 16), slot_rows)
            query = projected_ref[rows, 0:feature]
            key = projected_ref[rows, low_key : 2 * feature].astype(f32)[:, feature - low_key :]
            key = key.astype(bf16)
            value = projected_ref[rows, 2 * feature : used]
            matches = label_col[j][:, 0:1] == label_row[j]
            spans = [(t, min(t + 128, feature)) for t in range(0, feature, 128)]
            totals = [jnp.zeros((slot_rows, high - low), f32) for low, high in spans]
            for h in range(heads):
                low = h * HEAD // 128 * 128
                high = min(((h + 1) * HEAD + 127) // 128 * 128, feature)
                lane = low + lax.broadcasted_iota(jnp.int32, (slot_rows, high - low), 1)
                inside = (lane >= h * HEAD) & (lane < (h + 1) * HEAD)
                zero = jnp.zeros((slot_rows, high - low), bf16)
                scores = lax.dot_general(
                    jnp.where(inside, query[:, low:high], zero),
                    key[:, low:high],
                    (((1,), (1,)), ((), ())),
                    preferred_element_type=f32,
                )
                scores = jnp.where(matches, scores * scale, -jnp.inf)
                weights = jnp.exp(scores - jnp.max(scores, axis=-1, keepdims=True))
                inverse = 1.0 / jnp.sum(weights, axis=-1, keepdims=True)
                probabilities = (weights * inverse).astype(bf16)
                y = jnp.dot(
                    probabilities,
                    jnp.where(inside, value[:, low:high], zero),
                    preferred_element_type=f32,
                )
                for s, (a, b) in enumerate(spans):
                    if low <= a and b <= high:
                        totals[s] = totals[s] + y[:, a - low : b - low]
            shifted = jnp.concatenate(
                [jnp.zeros((slot_rows, used - low_out), f32)] + totals, axis=-1
            )
            attended_ref[rows, :] = shifted.astype(bf16)
            return carry

        lax.fori_loop(0, per, one_slot, 0)

        def out_column(t, carry):
            at = pl.ds(pl.multiple_of(t * column, column), column)
            residual_ref[:, at] = residual_ref[:, at] + lax.dot_general(
                attended_ref[...],
                w_attention[group, at, low_out:total_width],
                (((1,), (1,)), ((), ())),
                preferred_element_type=f32,
            )
            return carry

        lax.fori_loop(0, depth // column, out_column, 0)
        return carry

    lax.fori_loop(0, groups, one_group, 0)

    norm_tile = tile_of(piece_rows, 32)
    for h in range(pieces):

        def norm_some(i, carry, h=h):
            rows = pl.ds(pl.multiple_of(i * norm_tile, norm_tile), norm_tile)
            at = pl.ds(pl.multiple_of(h * piece_rows + i * norm_tile, norm_tile), norm_tile)
            blocks[0, h, rows, :] = norm_rows(residual_ref[at, :], gain_ref[1:2], shift_ref[1:2])
            return carry

        lax.fori_loop(0, piece_rows // norm_tile, norm_some, 0)

    def slot_of(k, h):
        return k if h == 0 or k in (0, 3) else 3 - k

    def out_copy(k, h):
        q = slot_of(k, h)
        at = q * pieces + h
        return remote(blocks.at[0, h], blocks.at[q, h], send_a.at[at], recv_a.at[at], peer(k))

    def back_copy(k, h):
        q = slot_of(k, h)
        at = q * pieces + h
        return remote(parts.at[q, h], backs.at[q, h], send_b.at[at], recv_b.at[at], peer(k))

    def forward(h):
        at = 3 * pieces + h
        return remote(blocks.at[1, h], blocks.at[3, h], send_a.at[at], recv_a.at[at], peer(2 - h))

    def across(h):
        at = 3 * pieces + h
        return remote(parts.at[3, h], relay.at[h], send_b.at[at], recv_b.at[at], peer(1 + h))

    first_pair = ((1, 0), (2, 1))
    second_pair = ((1, 1), (2, 0))
    for k, h in first_pair + second_pair:
        out_copy(k, h).start()

    @pl.when(edge_plane)
    def _():
        mlp_held(0, 3)

    def mlp_here(j):
        for plane in range(planes):
            at = w_mlp.at[0, pl.ds(0, shard_rows), :]
            remote(
                at, at, mlp_twin.at[0], mlp_twin_recv.at[j * planes + plane], twin
            ).wait_recv()

    mlp_here(0)
    pair_rows = pieces * piece_rows

    def mlp_step(i, carry):
        q = lax.rem(i + 1, 4)

        @pl.when(i == 0)
        def _():
            mlp_held(1, 2)

            @pl.when(jnp.logical_not(edge_plane))
            def _():
                mlp_held(1, 3)

            for k, h in first_pair:
                out_copy(k, h).wait_recv()
            forward(0).start()
            forward(1).start()

        @pl.when(i == 1)
        def _():
            for k, h in second_pair:
                out_copy(k, h).wait_recv()

        @pl.when(i == 2)
        def _():
            for h in range(2):
                forward(h).wait_recv()

        def up(t, carry):
            at = pl.ds(pl.multiple_of(t * column, column), column)
            x = blocks[q].reshape(pair_rows, depth)
            y = jnp.dot(x, w_mlp[0, :, at], preferred_element_type=f32) + b_up_ref[:, at]
            y = 0.5 * y * (1.0 + lax.erf(y * math.sqrt(0.5)))
            hidden_ref[:, at] = y.astype(bf16)
            return carry

        lax.fori_loop(0, hidden_ref.shape[1] // column, up, 0)

        @pl.when(i == 0)
        def _():
            @pl.when(edge_plane)
            def _():
                mlp_held(1, 3)

            mlp_here(1)

        def down(t, carry):
            at = pl.ds(pl.multiple_of(t * column, column), column)
            y = lax.dot_general(
                hidden_ref[...],
                w_mlp[1, at, :],
                (((1,), (1,)), ((), ())),
                preferred_element_type=f32,
            ).astype(bf16)
            for h in range(pieces):
                parts[q, h, :, at] = y[h * piece_rows : (h + 1) * piece_rows]
            return carry

        lax.fori_loop(0, depth // column, down, 0)

        @pl.when(i == 0)
        def _():
            for k, h in first_pair:
                back_copy(k, h).start()

        @pl.when(i == 2)
        def _():
            for h in range(2):
                across(h).start()

        return carry

    lax.fori_loop(0, 4, mlp_step, 0)
    for k, h in second_pair:
        across(h).wait_recv()

        def add(i, carry, h=h):
            rows = pl.ds(pl.multiple_of(i * norm_tile, norm_tile), norm_tile)
            parts[2, h, rows, :] = (
                parts[2, h, rows, :].astype(f32) + relay[h, rows, :].astype(f32)
            ).astype(bf16)
            return carry

        lax.fori_loop(0, piece_rows // norm_tile, add, 0)
        back_copy(k, h).start()
    for k, h in first_pair + second_pair:
        back_copy(k, h).wait_recv()
    for h in range(pieces):

        def finish(i, carry, h=h):
            rows = pl.ds(pl.multiple_of(i * norm_tile, norm_tile), norm_tile)
            at = pl.ds(pl.multiple_of(h * piece_rows + i * norm_tile, norm_tile), norm_tile)
            total = residual_ref[at, :] + b_down_ref[...] + parts[0, h, rows, :].astype(f32)
            for q in (1, 2):
                total = total + backs[q, h, rows, :].astype(f32)
            live = label_col[h, rows, :][:, 0:1] >= 0
            out_ref[at, :] = jnp.where(live, total, 0.0).astype(bf16)
            return carry

        lax.fori_loop(0, piece_rows // norm_tile, finish, 0)

    for h in range(2):
        forward(h).wait_send()
        across(h).wait_send()
        for k in (1, 2):
            out_copy(k, h).wait_send()
            back_copy(k, h).wait_send()
    for k in range(1, groups):
        bias_copy(k).wait_send()
    for g in range(groups):

        @pl.when(mp != g)
        def _():
            for i in range(half_images):
                token_copy(g, i).wait_send()

    def slot_sent(dest, carry):
        @pl.when(jnp.logical_not(jnp.logical_and(is_home, dest == dp)))
        def _():
            slot_copy(dest).wait_send()

        return carry

    lax.fori_loop(0, shards, slot_sent, 0)
    att_own(False)
    att_end(False)
    for j in range(2):
        mlp_own(j, False)
        mlp_end(j, False)
    for p in range(planes):
        plane = arrival(p)
        for g in range(groups):
            att_to_twin(g, plane).wait_send()
        for j in range(2):
            mlp_to_twin(j, plane).wait_send()
        for k in (1, 2):
            att_over(k, mp, plane, 0).wait_send()
        k = 1 + p % 2
        att_over(3 - k, flip(mp, k, groups), plane, 1).wait_send()


def one_kernel(
    patches,
    position,
    keep,
    counts,
    offsets,
    ln_gain,
    ln_bias,
    w_qkv,
    b_qkv,
    w_o,
    b_o,
    w_up,
    b_up,
    w_down,
    b_down,
):
    images, _, depth = patches.shape
    keep_most = keep.shape[1]
    shards = lax.axis_size("dp")
    groups = lax.axis_size("mp")
    slot_rows = slot_size(images * groups, shards, keep_most)
    per = shards // groups
    feature = depth // groups
    planes = shards // 2
    rows = per * slot_rows
    used = 3 * feature
    padded = (used + 255) // 256 * 256
    hidden = w_up.shape[2]
    shard_width = used + w_o.shape[1]
    some = (images // 2) * keep_most
    bf16 = jnp.bfloat16
    i32 = jnp.int32
    vmem = pl.BlockSpec(memory_space=pltpu.VMEM)
    smem = pl.BlockSpec(memory_space=pltpu.SMEM)
    dma = pltpu.SemaphoreType.DMA
    buffer = pltpu.VMEM((groups, per, slot_rows, depth), bf16)
    return pl.pallas_call(
        functools.partial(layer_kernel, shards, groups),
        out_shape=jax.ShapeDtypeStruct((rows, depth), bf16),
        in_specs=[pl.BlockSpec(memory_space=pl.ANY), vmem, vmem, smem, smem] + [vmem] * 10,
        out_specs=vmem,
        scratch_shapes=[
            pltpu.VMEM(patches.shape, bf16),
            pltpu.VMEM((groups, some, 2 * feature), bf16),
            pltpu.VMEM((groups, some, 2 * feature), bf16),
            pltpu.VMEM((shards, slot_rows // 2, 2 * feature), bf16),
            pltpu.VMEM((shards, slot_rows // 2, 2 * feature), bf16),
            pltpu.VMEM((groups, depth, shard_width), bf16),
            pltpu.VMEM((groups, 8, padded), jnp.float32),
            pltpu.VMEM((2, depth, hidden), bf16),
            pltpu.VMEM((per, slot_rows, 128), i32),
            pltpu.VMEM((per, 1, slot_rows), i32),
            pltpu.VMEM((2, 1, groups * some), i32),
            pltpu.VMEM((rows, depth), bf16),
            pltpu.VMEM((rows, padded), bf16),
            pltpu.VMEM((rows, shard_width - used // 128 * 128), bf16),
            pltpu.VMEM((rows, depth), jnp.float32),
            buffer,
            buffer,
            buffer,
            pltpu.VMEM((per, slot_rows, depth), bf16),
            pltpu.VMEM((rows, hidden), bf16),
            dma((images,)),
            dma((1,)),
            dma((groups * images // 2,)),
            dma((groups * images // 2,)),
            dma((shards,)),
            dma((shards,)),
            dma((groups,)),
            dma((groups,)),
            dma((8,)),
            dma((6 * planes,)),
            dma((groups * planes,)),
            dma((groups * planes,)),
            dma((groups * planes,)),
            dma((16,)),
            dma((2 * planes,)),
            dma((2 * planes,)),
            dma((2 * planes,)),
            dma((groups * per,)),
            dma((groups * per,)),
            dma((groups * per,)),
            dma((groups * per,)),
        ],
        compiler_params=pltpu.CompilerParams(
            collective_id=3, has_side_effects=True, vmem_limit_bytes=60 * 1024 * 1024
        ),
        cost_estimate=pl.CostEstimate(flops=100_000_000_000, bytes_accessed=0, transcendentals=0),
        name="layer",
    )(
        patches,
        position,
        keep,
        counts,
        offsets,
        ln_gain[0],
        ln_bias[0],
        w_qkv[0],
        b_qkv[0],
        w_o[0],
        b_o,
        w_up[0],
        b_up,
        w_down[0],
        b_down,
    )


def solution(mesh):
    in_specs = (
        P(("dp", "mp"), None, None),
        P(),
        P(("dp", "mp"), None),
        P(),
        P(),
        P(),
        P(),
        P(None, None, "dp", "mp"),
        P(None, None, "mp"),
        P(None, "mp", "dp"),
        P(),
        P(None, "dp", "mp"),
        P(None, "mp"),
        P(None, "mp", "dp"),
        P(),
    )
    out_specs = P(("dp", "mp"), None)
    square = mesh.shape["mp"] == 4 and mesh.shape["dp"] == 8
    return jax.shard_map(
        one_kernel if square else per_device, mesh=mesh, in_specs=in_specs, out_specs=out_specs, check_vma=False
    )
```
